256 devices in a mesh: row: 4 (over y), sa: 4 (over x), ha: 16 (over z, core).
Axes of the slice: x: 4, y: 4, z: 8, core: 2. Of those that a mesh axis runs over, the one named last changes fastest.
Arguments:
- records: float32 [64, 16, 65536], P(None, 'sa', ('row', 'ha')), parts along dimension 2, may hold values from -6 to 6
- halo_mass: float32 [16, 65536], P('sa', ('row', 'ha')), parts along dimension 1, may hold values from 0.1 to 10
- forest_id: int32 [16, 65536], P('sa', ('row', 'ha')), parts along dimension 1, may hold values from 0 to 8191, as said below
- dest_block: int32 [16, 65536], P('sa', ('row', 'ha')), parts along dimension 1, may hold values from 0 to 2559, as said below
- dest_slot: int32 [16, 65536], P('sa', ('row', 'ha')), parts along dimension 1, may hold values from 0 to 127
Outputs:
- blocks: float32 [64, 10240, 128], P(None, ('row', 'sa', 'ha')), parts along dimension 1
- block_mass: float32 [10240, 128], P(('row', 'sa', 'ha')), parts along dimension 0
- forest_mass: float32 [32768], P(('row', 'sa', 'ha')), parts along dimension 0
- forest_mean: float32 [64, 32768], P(None, ('row', 'sa', 'ha')), parts along dimension 1
- forest_second: float32 [64, 32768], P(None, ('row', 'sa', 'ha')), parts along dimension 1
The draws below stay inside these ranges and needn't reach their ends.
There are 4 independent parts, one for each index of `row`. The reference program is written for one: setup_inputs(seed, part) draws one part's arguments, and reference() takes and returns one part's arrays. A program takes and returns all parts, laid end to end along the dimension named above; each array names one. Nothing has to cross between parts.
Inputs may be any that keep to these rules, and one draw needn't show every extreme that they name: The pairs (dest_block, dest_slot) are distinct over all halos. Block b lies on the device of index b // 40 of sa+ha (sa slowest), and forest f is owned by the device of index f // 128; every halo goes to a block of its forest's owner. On each device the used slots are the first ones in block-then-slot order, and every forest has at least one halo. `forest_id`: of the halos of one device (one index of sa and one of ha), at most 88 go to blocks of one device; in every draw some pair of devices reaches 88, and some device has all its 5120 slots used.
All inputs are finite; a program needn't handle non-finite values.
Results may differ from the reference program's by a relative error of at most 0.0003.
Values sent between devices are 32-bit elements; how exact they have to be, the bound alone decides.
No kernel may reach another device: no remote copies, remote signals or barrier semaphores. Data moves between devices by JAX's collectives and lax.ppermute only.
A program may use at most 64 MiB of HBM per device.

```python
import math
import jax
import jax.numpy as jnp
from jax import lax

FIELDS = 64
S_DEV = 4
H_DEV = 1024
FOR_DEV = 128
SNAPS = 16
HALOS = 16384
BLK_DEV = 40
NBLK = 2560
NFOR = 8192
N_SA = 4
N_HA = 16


def route_table(key):
    peer_count = N_SA * N_HA
    local_count = S_DEV * H_DEV
    pair_mean = local_count // peer_count
    entries_all = peer_count * local_count
    slots_dev = BLK_DEV * 128
    half_peers = peer_count // 2
    key_list = jax.random.split(jax.random.fold_in(key, 91), 8)
    lift_up = jax.random.randint(key_list[0], (half_peers,), 0, pair_mean // 4 + 1)
    lift_up = lift_up.at[0].set(pair_mean // 4)
    load_in = pair_mean + jnp.concatenate([lift_up, -lift_up])[jax.random.permutation(key_list[1], peer_count)]
    wobble = jax.random.randint(key_list[2], (half_peers,), -(pair_mean // 8), pair_mean // 8 + 1)
    wobble = wobble.at[0].set(pair_mean // 8)
    offsets = jnp.concatenate([wobble, -wobble])
    shift_dst = jax.random.permutation(key_list[3], peer_count)
    shift_src = jax.random.permutation(key_list[4], peer_count)
    pair_counts = load_in[None, :] + offsets[(shift_dst[None, :] - shift_src[:, None]) % peer_count]
    flat_counts = pair_counts.T.reshape(-1)
    pair_ends = jnp.cumsum(flat_counts).astype(jnp.int32)
    entry_index = jnp.arange(entries_all, dtype=jnp.int32)
    pair_of = jnp.searchsorted(pair_ends, entry_index, side='right').astype(jnp.int32)
    dest_dev = pair_of // peer_count
    src_dev = pair_of % peer_count
    inbound = (peer_count * load_in).astype(jnp.int32)
    recv_start = (jnp.cumsum(inbound) - inbound).astype(jnp.int32)
    shuffle_in = jax.random.permutation(key_list[5], entries_all).astype(jnp.int32)
    order_in = jnp.argsort(dest_dev * entries_all + shuffle_in, stable=True)
    place_in = jnp.zeros((entries_all,), jnp.int32).at[order_in].set(entry_index)
    position = place_in - recv_start[dest_dev]
    shuffle_out = jax.random.permutation(key_list[6], entries_all).astype(jnp.int32)
    order_out = jnp.argsort(src_dev * entries_all + shuffle_out, stable=True)
    place_out = jnp.zeros((entries_all,), jnp.int32).at[order_out].set(entry_index)
    local_pos = place_out - src_dev * local_count
    heights = jax.random.randint(key_list[7], (peer_count, FOR_DEV), 1, 8) ** 2
    climb_sum = jnp.cumsum(heights, axis=1)
    spare_slots = inbound - FOR_DEV
    starts = jnp.arange(FOR_DEV, dtype=jnp.int32)[None, :] + spare_slots[:, None] * (climb_sum - heights) // climb_sum[:, -1:]
    global_starts = (recv_start[:, None] + starts).reshape(-1).astype(jnp.int32)
    forest = (jnp.searchsorted(global_starts, place_in, side='right') - 1).astype(jnp.int32)
    global_slot = dest_dev * slots_dev + position
    snap_index = src_dev // N_HA * S_DEV + local_pos // H_DEV
    halo_index = src_dev % N_HA * H_DEV + local_pos % H_DEV

    def spread(values):
        return jnp.zeros((SNAPS, HALOS), jnp.int32).at[snap_index, halo_index].set(values.astype(jnp.int32))
    return (spread(forest), spread(global_slot // 128), spread(global_slot % 128))


def draw_forest_id(key, part):
    return route_table(key)[0]


def draw_dest_block(key, part):
    return route_table(key)[1]


def draw_dest_slot(key, part):
    return route_table(key)[2]


def block_levels(stream_key, extent, cuts, least, high):
    def one(dim, shards_of):
        steps = jax.random.uniform(jax.random.fold_in(jax.random.fold_in(stream_key, 6), dim), (shards_of,), jnp.float32, least / len(cuts), high / len(cuts))
        return jnp.repeat(jnp.exp(steps), extent[dim] // shards_of).reshape((-1,) + (1,) * (len(extent) - dim - 1))

    loudness = one(*cuts[0])
    for cut in cuts[1:]:
        loudness = loudness * one(*cut)
    return loudness


def centred(key, extent, scale, most, pieces=(), kind=jnp.bfloat16):
    values = jax.random.normal(key, extent, jnp.float32) * scale
    if len(pieces) > 0:
        values = block_levels(key, extent, pieces, -0.22, 0.18) * values
    return jnp.clip(values, min=-most, max=most).astype(kind)


def setup_inputs(seed: int = 0, part: int = 0) -> dict:
    keys = jax.random.split(jax.random.key(seed), 6)
    part_splits = jax.random.split(jax.random.fold_in(keys[5], part), 6)
    return {
        "records": centred(part_splits[0], (FIELDS, SNAPS, HALOS), 1.0, 6.0, ((1, 4), (2, 16)), jnp.float32),
        "halo_mass": jnp.clip(jnp.exp(math.log(10.0) - 4.6051702 * jax.random.uniform(part_splits[1], (SNAPS, HALOS), jnp.float32) ** block_levels(part_splits[1], (SNAPS, HALOS), ((0, 4), (1, 16)), -0.2, 0.2)), 0.1, 10.0),
        "forest_id": draw_forest_id(jax.random.fold_in(jax.random.fold_in(keys[5], part), 71), part),
        "dest_block": draw_dest_block(jax.random.fold_in(jax.random.fold_in(keys[5], part), 71), part),
        "dest_slot": draw_dest_slot(jax.random.fold_in(jax.random.fold_in(keys[5], part), 71), part),
    }


def reference(records, halo_mass, forest_id, dest_block, dest_slot):
    fields = records.shape[0]
    flat = records.reshape(fields, -1)
    weights_in = halo_mass.reshape(-1)
    home = (dest_block * 128 + dest_slot).reshape(-1).astype(jnp.int32)
    slot_total = NBLK * 128
    blocks = jnp.zeros((fields, slot_total), jnp.float32).at[:, home].set(flat)
    block_mass = jnp.zeros((slot_total,), jnp.float32).at[home].set(weights_in)
    forest_in = forest_id.reshape(-1).astype(jnp.int32)
    weight = jax.ops.segment_sum(weights_in, forest_in, NFOR)

    def per_field(values):
        scaled = weights_in * values
        return (jax.ops.segment_sum(scaled, forest_in, NFOR),
                jax.ops.segment_sum(scaled * values, forest_in, NFOR))

    first_sum, square_sum = lax.map(per_field, flat)
    mass_total = jnp.sum(weights_in)
    forest_mass = weight * (NFOR / mass_total)
    return (blocks.reshape(fields, NBLK, 128), block_mass.reshape(NBLK, 128),
            forest_mass, first_sum / weight[None, :], square_sum / weight[None, :])
```

```python
import functools

import jax
import jax.numpy as jnp
from jax import lax
from jax.experimental import pallas as pl
from jax.experimental.pallas import tpu as pltpu
from jax.sharding import Mesh
from jax.sharding import PartitionSpec as P

FIELDS = 64
FOR_DEV = 128
BLK_DEV = 40
SLOTS = BLK_DEV * 128
PEERS = 64
CAP = 88
ROWS = 48
SA_HA = ("sa", "ha_0", "ha_1")
ROW_HA = ("row", "ha_0", "ha_1")
ROW_SA_HA = ("row", "sa", "ha_0", "ha_1")


def iota(shape, dim):
    return lax.broadcasted_iota(jnp.int32, shape, dim)


def owner_of(block):
    return lax.shift_right_logical(block * 1639, 16)


def pack_kernel(rec, mass, forest, block, slot, out, placed, tile_a, tile_b, target_v, target_s, sem):
    snaps, halos = mass.shape
    per_snap = halos // 128
    before = (iota((256, 384), 0) < iota((256, 384), 1)) | (iota((256, 384), 1) >= 256)
    before = before.astype(jnp.float32).astype(jnp.bfloat16)
    peer = iota((PEERS, 256), 0)
    base = jnp.zeros((PEERS, 128), jnp.float32)
    for s in range(snaps):
        for q in range(halos // 256):
            own = owner_of(block[s : s + 1, 256 * q : 256 * q + 256])
            member = peer == own
            counts = jnp.dot(
                member.astype(jnp.float32).astype(jnp.bfloat16), before, preferred_element_type=jnp.float32
            )
            rank = counts[:, :256] + jnp.concatenate([base, base], axis=1)
            rank = jnp.sum(jnp.where(member, rank, 0.0), axis=0, keepdims=True)
            base = base + counts[:, 256:]
            target = own * CAP + rank.astype(jnp.int32)
            row = s * per_snap + 2 * q
            target_v[row : row + 1, :] = target[:, :128]
            target_v[row + 1 : row + 2, :] = target[:, 128:]
    copy = pltpu.make_async_copy(target_v, target_s, sem)
    copy.start()

    def clear(k, carry):
        placed[pl.ds(pl.multiple_of(k * 64, 64), 64), :] = jnp.zeros((64, 128), jnp.float32)
        return carry

    lax.fori_loop(0, PEERS * CAP // 64, clear, 0)
    copy.wait()
    first = iota((8, 128), 0) == 0
    none8 = jnp.zeros((8, 128), jnp.float32)

    def turn(s, group, tile):
        cols = pl.ds(pl.multiple_of(group * 128, 128), 128)
        blk = block[s : s + 1, cols]
        local = (blk - owner_of(blk) * BLK_DEV) * 128 + slot[s : s + 1, cols] + 1
        here = forest[s : s + 1, cols] & (FOR_DEV - 1)

        def label(row):
            return jnp.where(first, jnp.broadcast_to(row, (8, 128)), 0.0)

        stack = jnp.concatenate(
            [
                rec[:, s, cols],
                label(mass[s : s + 1, cols]),
                none8,
                label(local.astype(jnp.float32)),
                none8,
                label(here.astype(jnp.float32)),
                none8,
                none8,
                none8,
            ],
            axis=0,
        )
        tile[...] = stack.T

    def spread(group, tile):
        for i in range(128):
            placed[pl.ds(target_s[group, i], 1), :] = tile[i : i + 1, :]

    turn(0, 0, tile_a)
    for s in range(snaps):

        def step(k, carry):
            turn(s, 2 * k + 1, tile_b)
            spread(s * per_snap + 2 * k, tile_a)
            turn(s, 2 * k + 2, tile_a)
            spread(s * per_snap + 2 * k + 1, tile_b)
            return carry

        lax.fori_loop(0, per_snap // 2 - 1, step, 0)
        turn(s, per_snap - 1, tile_b)
        spread(s * per_snap + per_snap - 2, tile_a)
        if s + 1 < snaps:
            turn(s + 1, 0, tile_a)
        spread(s * per_snap + per_snap - 1, tile_b)

    lane = iota((8, 128), 1)
    low = lane < FIELDS
    total = jnp.sum(jnp.sum(mass[...], axis=0, keepdims=True), axis=1, keepdims=True)

    def squeeze(p, carry):
        start = p * CAP
        tiles = [placed[pl.ds(pl.multiple_of(start + 8 * v, 8), 8), :] for v in range(CAP // 8)]
        labels = jnp.where(lane == 127, jnp.broadcast_to(total, (8, 128)), 0.0)
        for v in range(CAP // 8):
            own = jnp.where(low, 0.0, tiles[v])
            labels = labels + (pltpu.roll(own, v, 1) if v else own)
        for v in range(5):
            out[p, 8 * v : 8 * v + 8, :] = jnp.where(low, tiles[v], pltpu.roll(tiles[v + 6], 64, 1))
        out[p, 40:48, :] = jnp.where(low, tiles[5], labels)
        return carry

    lax.fori_loop(0, PEERS, squeeze, 0)


def place_kernel(
    msg, blocks, block_mass, fmass, fmean, fsecond, placed, tile_a, tile_b, slot_v, slot_s, sem
):
    lane = iota((8, 128), 1)
    low = lane < FIELDS
    slot_lane = (lane >= 80) & (lane < 80 + CAP // 8)
    total = jnp.zeros((8, 128), jnp.float32)
    for g in range(PEERS // 8):
        acc = jnp.zeros((8, 128), jnp.float32)
        for k in range(8):
            labels = msg[8 * g + k, 40:48, :]
            total = total + labels
            acc = acc + pltpu.roll(jnp.where(slot_lane, labels, 0.0), (16 * k - 80) % 128, 1)
        index = acc.astype(jnp.int32)
        slot_v[8 * g : 8 * g + 8, :] = jnp.where(index == 0, SLOTS, index - 1)
    copy = pltpu.make_async_copy(slot_v, slot_s, sem)
    copy.start()

    def clear(k, carry):
        placed[pl.ds(pl.multiple_of(k * 64, 64), 64), :] = jnp.zeros((64, 128), jnp.float32)
        return carry

    lax.fori_loop(0, SLOTS // 64, clear, 0)
    copy.wait()

    def turn(p, tile):
        labels = msg[p, 40:48, :]
        for v in range(CAP // 8):
            own = msg[p, 8 * v : 8 * v + 8, :] if v < 6 else pltpu.roll(msg[p, 8 * v - 48 : 8 * v - 40, :], 64, 1)
            tile[8 * v : 8 * v + 8, :] = jnp.where(low, own, pltpu.roll(labels, (128 - v) % 128, 1) if v else labels)

    def spread(p, tile):
        row = p // 8 * 8
        col = p % 8 * 16
        for r in range(CAP):
            placed[pl.ds(slot_s[row + r % 8, col + r // 8], 1), :] = tile[r : r + 1, :]

    turn(0, tile_a)

    def step(k, carry):
        turn(2 * k + 1, tile_b)
        spread(2 * k, tile_a)
        turn(jnp.minimum(2 * k + 2, PEERS - 1), tile_a)
        spread(2 * k + 1, tile_b)
        return carry

    lax.fori_loop(0, PEERS // 2, step, 0)

    owned = iota((FOR_DEV, 128), 0)

    def finish(b, acc):
        view = placed[pl.ds(pl.multiple_of(b * 128, 128), 128), :].T
        x = view[:FIELDS]
        m = view[FIELDS : FIELDS + 1]
        blocks[:, b, :] = x
        block_mass[pl.ds(b, 1), :] = m
        where = view[96:97].astype(jnp.int32)
        member = (owned == where).astype(jnp.float32).astype(jnp.bfloat16)
        scaled = m * x
        terms = jnp.concatenate([scaled, scaled * x, jnp.broadcast_to(m, (8, 128))], axis=0)
        for _ in range(3):
            piece = terms.astype(jnp.bfloat16)
            terms = terms - piece.astype(jnp.float32)
            acc = acc + lax.dot_general(
                piece, member, (((1,), (1,)), ((), ())), preferred_element_type=jnp.float32
            )
        return acc

    acc = lax.fori_loop(0, BLK_DEV, finish, jnp.zeros((2 * FIELDS + 8, FOR_DEV), jnp.float32))
    weight = acc[2 * FIELDS : 2 * FIELDS + 1]
    mass_total = jnp.broadcast_to(total[0:1, 127:128], (1, FOR_DEV))
    fmass[...] = weight * (FOR_DEV * PEERS / mass_total)
    fmean[...] = acc[:FIELDS] / weight
    fsecond[...] = acc[FIELDS : 2 * FIELDS] / weight


def pack(records, halo_mass, forest_id, dest_block, dest_slot):
    groups = halo_mass.size // 128
    return pl.pallas_call(
        pack_kernel,
        out_shape=jax.ShapeDtypeStruct((PEERS, ROWS, 128), jnp.float32),
        in_specs=[pl.BlockSpec(memory_space=pltpu.VMEM)] * 5,
        out_specs=pl.BlockSpec(memory_space=pltpu.VMEM),
        scratch_shapes=[
            pltpu.VMEM((PEERS * CAP, 128), jnp.float32),
            pltpu.VMEM((128, 128), jnp.float32),
            pltpu.VMEM((128, 128), jnp.float32),
            pltpu.VMEM((groups, 128), jnp.int32),
            pltpu.SMEM((groups, 128), jnp.int32),
            pltpu.SemaphoreType.DMA,
        ],
        name="pack",
    )(records, halo_mass, forest_id, dest_block, dest_slot)


def place(msg):
    f32 = jnp.float32
    return pl.pallas_call(
        place_kernel,
        out_shape=(
            jax.ShapeDtypeStruct((FIELDS, BLK_DEV, 128), f32),
            jax.ShapeDtypeStruct((BLK_DEV, 128), f32),
            jax.ShapeDtypeStruct((1, FOR_DEV), f32),
            jax.ShapeDtypeStruct((FIELDS, FOR_DEV), f32),
            jax.ShapeDtypeStruct((FIELDS, FOR_DEV), f32),
        ),
        in_specs=[pl.BlockSpec(memory_space=pltpu.VMEM)],
        out_specs=(pl.BlockSpec(memory_space=pltpu.VMEM),) * 5,
        scratch_shapes=[
            pltpu.VMEM((SLOTS + 8, 128), f32),
            pltpu.VMEM((CAP, 128), f32),
            pltpu.VMEM((CAP, 128), f32),
            pltpu.VMEM((PEERS, 128), jnp.int32),
            pltpu.SMEM((PEERS, 128), jnp.int32),
            pltpu.SemaphoreType.DMA,
        ],
        name="place",
    )(msg)


def on_device(records, halo_mass, forest_id, dest_block, dest_slot):
    outbox = pack(records, halo_mass, forest_id, dest_block, dest_slot)
    inbox = lax.all_to_all(outbox, SA_HA, split_axis=0, concat_axis=0, tiled=True)
    blocks, block_mass, fmass, fmean, fsecond = place(inbox)
    return blocks, block_mass, fmass.reshape(FOR_DEV), fmean, fsecond


def solution(mesh):
    split = Mesh(
        mesh.devices.reshape(mesh.shape["row"], mesh.shape["sa"], 8, 2),
        ("row", "sa", "ha_0", "ha_1"),
    )
    in_specs = (
        P(None, "sa", ROW_HA),
        P("sa", ROW_HA),
        P("sa", ROW_HA),
        P("sa", ROW_HA),
        P("sa", ROW_HA),
    )
    out_specs = (
        P(None, ROW_SA_HA, None),
        P(ROW_SA_HA, None),
        P(ROW_SA_HA),
        P(None, ROW_SA_HA),
        P(None, ROW_SA_HA),
    )
    return jax.shard_map(
        on_device, mesh=split, in_specs=in_specs, out_specs=out_specs, check_vma=False
    )
```

```python
import jax
import jax.numpy as jnp
from jax import lax
from jax.experimental import pallas as pl
from jax.experimental.pallas import tpu as pltpu
from jax.sharding import Mesh
from jax.sharding import PartitionSpec as P

FIELDS = 64
FOR_DEV = 128
BLK_DEV = 40
SLOTS = BLK_DEV * 128
PEERS = 64
CAP = 88
ROWS = 48
VMEM_LIMIT = 24 * 1024 * 1024
EXCHANGE = ("core", "sa", "z0", "z1", "z2")
ROW_HA = ("row", "z2", "z1", "z0", "core")
ROW_SA_HA = ("row", "sa", "z2", "z1", "z0", "core")


def iota(shape, dim):
    return lax.broadcasted_iota(jnp.int32, shape, dim)


def owner_of(block):
    return lax.shift_right_logical(block * 1639, 16)


def position_of(owner):
    core = (owner & 1) << 5
    plane = lax.shift_right_logical(owner, 4) << 3
    turned = ((owner & 2) << 1) | lax.shift_right_logical(owner & 4, 1) | lax.shift_right_logical(owner & 8, 3)
    return core | plane | turned


def pack_kernel(
    rec_hbm, mass, forest, block, slot, out, placed, rec, labels, tiles, target_v, target_s, rec_sem, sems
):
    snaps, halos = mass.shape
    groups = snaps * halos // 128
    rec_copy = pltpu.make_async_copy(rec_hbm, rec, rec_sem)
    rec_copy.start()
    before = (iota((256, 384), 0) < iota((256, 384), 1)) | (iota((256, 384), 1) >= 256)
    before = before.astype(jnp.float32).astype(jnp.bfloat16)
    peer = iota((PEERS, 256), 0)
    base = jnp.zeros((PEERS, 128), jnp.float32)
    line = iota((8, 128), 0)

    for q in range(halos // 256):
        for s in range(snaps):
            cols = slice(256 * q, 256 * q + 256)
            blk = block[s : s + 1, cols]
            own = owner_of(blk)
            place = position_of(own)
            member = peer == place
            counts = jnp.dot(
                member.astype(jnp.float32).astype(jnp.bfloat16), before, preferred_element_type=jnp.float32
            )
            rank = counts[:, :256] + jnp.concatenate([base, base], axis=1)
            rank = jnp.sum(jnp.where(member, rank, 0.0), axis=0, keepdims=True)
            base = base + counts[:, 256:]
            target = place * CAP + rank.astype(jnp.int32)
            local = ((blk - own * BLK_DEV) * 128 + slot[s : s + 1, cols] + 1).astype(jnp.float32)
            here = (forest[s : s + 1, cols] & (FOR_DEV - 1)).astype(jnp.float32)
            heavy = mass[s : s + 1, cols]
            for h in range(2):
                part = slice(128 * h, 128 * h + 128)
                group = 8 * q + 4 * h + s
                target_v[group : group + 1, :] = target[:, part]
                tile = jnp.where(line == 0, jnp.broadcast_to(heavy[:, part], (8, 128)), 0.0)
                tile = jnp.where(line == 1, jnp.broadcast_to(local[:, part], (8, 128)), tile)
                tile = jnp.where(line == 2, jnp.broadcast_to(here[:, part], (8, 128)), tile)
                labels[8 * group : 8 * group + 8, :] = tile

    def index_copy(k, buf):
        return pltpu.make_async_copy(
            target_v.at[pl.ds(pl.multiple_of(8 * k, 8), 8), :], target_s[buf], sems.at[buf]
        )

    index_copy(0, 0).start()
    index_copy(1, 1).start()
    for tile in tiles:
        tile[...] = jnp.zeros_like(tile)

    def clear(k, carry):
        placed[pl.ds(pl.multiple_of(k * 128, 128), 128), :] = jnp.zeros((128, 128), jnp.float32)
        return carry

    lax.fori_loop(0, PEERS * CAP // 128, clear, 0)
    rec_copy.wait()

    def turn(group, tile):
        stack = jnp.concatenate(
            [
                rec[pl.ds(group, FIELDS, stride=groups), :],
                labels[pl.ds(pl.multiple_of(8 * group, 8), 8), :],
            ],
            axis=0,
        )
        tile[:, : FIELDS + 8] = stack.T

    turn(0, tiles[0])

    def step(k, carry):
        for i in range(16):
            if i % 8 == 0:
                index_copy(0, i // 8).wait()
            after = jnp.minimum(16 * k + i + 1, groups - 1)
            turn(after, tiles[(i + 1) % 4])
            tile = tiles[i % 4]
            for r in range(128):
                placed[pl.ds(target_s[i // 8][i % 8, r], 1), :] = tile[r : r + 1, :]
            if i % 8 == 7:

                @pl.when(2 * k + i // 8 + 2 < groups // 8)
                def _():
                    index_copy(2 * k + i // 8 + 2, i // 8).start()

        return carry

    lax.fori_loop(0, groups // 16, step, 0)

    lane = iota((8, 128), 1)
    low = lane < FIELDS
    total = jnp.sum(jnp.sum(mass[...], axis=0, keepdims=True), axis=1, keepdims=True)
    corner = jnp.where(lane == 127, jnp.broadcast_to(total, (8, 128)), 0.0)

    def squeeze(k, carry):
        for h in range(4):
            p = 4 * k + h
            start = p * CAP
            rows = [placed[pl.ds(pl.multiple_of(start + 8 * v, 8), 8), :] for v in range(CAP // 8)]
            tags = corner
            for v in range(CAP // 8):
                own = jnp.where(low, 0.0, rows[v])
                tags = tags + (pltpu.roll(own, 4 * v, 1) if v else own)
            for v in range(5):
                out[p, 8 * v : 8 * v + 8, :] = jnp.where(low, rows[v], pltpu.roll(rows[v + 6], 64, 1))
            out[p, 40:48, :] = jnp.where(low, rows[5], tags)
        return carry

    lax.fori_loop(0, PEERS // 4, squeeze, 0)


def place_kernel(
    msg, blocks, block_mass, fmass, fmean, fsecond, placed, acc, tiles, slot_v, slot_s, sems
):
    lane = iota((8, 128), 1)
    low = lane < FIELDS
    slot_lane = (lane >= FIELDS) & (lane < FIELDS + 4 * (CAP // 8)) & (lane % 4 == 1)
    total = jnp.zeros((8, 128), jnp.float32)
    for g in range(PEERS // 8):
        index = jnp.zeros((8, 128), jnp.float32)
        for k in range(8):
            tags = msg[8 * g + k, 40:48, :]
            total = total + tags
            index = index + pltpu.roll(
                jnp.where(slot_lane, tags, 0.0), (64 * (k // 4) + k % 4 - 65) % 128, 1
            )
        index = index.astype(jnp.int32)
        slot_v[8 * g : 8 * g + 8, :] = jnp.where(index == 0, SLOTS, index - 1)

    def index_copy(g, buf):
        return pltpu.make_async_copy(
            slot_v.at[pl.ds(pl.multiple_of(8 * g, 8), 8), :], slot_s[buf], sems.at[buf]
        )

    index_copy(0, 0).start()
    index_copy(1, 1).start()

    def clear(k, carry):
        placed[pl.ds(pl.multiple_of(k * 128, 128), 128), :] = jnp.zeros((128, 128), jnp.float32)
        return carry

    lax.fori_loop(0, SLOTS // 128, clear, 0)
    acc[...] = jnp.zeros_like(acc)

    def turn(p, tile):
        tags = msg[p, 40:48, :]
        for v in range(CAP // 8):
            if v < 6:
                own = msg[p, 8 * v : 8 * v + 8, :]
            else:
                own = pltpu.roll(msg[p, 8 * v - 48 : 8 * v - 40, :], 64, 1)
            side = pltpu.roll(tags, 128 - 4 * v, 1) if v else tags
            tile[8 * v : 8 * v + 8, :] = jnp.where(low, own, side)

    turn(0, tiles[0])

    def step(k, carry):
        for i in range(16):
            if i % 8 == 0:
                index_copy(0, i // 8).wait()
            turn(jnp.minimum(16 * k + i + 1, PEERS - 1), tiles[(i + 1) % 4])
            tile = tiles[i % 4]
            for r in range(CAP):
                col = r // 8 * 4 + i % 8 % 4 + i % 8 // 4 * 64
                placed[pl.ds(slot_s[i // 8][r % 8, col], 1), :] = tile[r : r + 1, :]
            if i % 8 == 7:

                @pl.when(2 * k + i // 8 + 2 < PEERS // 8)
                def _():
                    index_copy(2 * k + i // 8 + 2, i // 8).start()

        return carry

    lax.fori_loop(0, PEERS // 16, step, 0)

    owned = iota((FOR_DEV, 128), 0)

    def finish(k, carry):
        highs, lows, members = [], [], []
        for h in range(4):
            b = 4 * k + h
            view = placed[pl.ds(pl.multiple_of(b * 128, 128), 128), :].T
            x = view[:FIELDS]
            m = view[FIELDS : FIELDS + 1]
            blocks[pl.ds(b, FIELDS, stride=BLK_DEV), :] = x
            block_mass[pl.ds(b, 1), :] = m
            forest = view[FIELDS + 2 : FIELDS + 3].astype(jnp.int32)
            members.append((owned == forest).astype(jnp.float32).astype(jnp.bfloat16))
            scaled = m * x
            terms = jnp.concatenate([scaled, scaled * x, jnp.broadcast_to(m, (8, 128))], axis=0)
            high = terms.astype(jnp.bfloat16)
            highs.append(high)
            lows.append((terms - high.astype(jnp.float32)).astype(jnp.bfloat16))
        member = jnp.concatenate(members, axis=1)
        for part in (highs, lows):
            acc[...] += lax.dot_general(
                jnp.concatenate(part, axis=1),
                member,
                (((1,), (1,)), ((), ())),
                preferred_element_type=jnp.float32,
            )
        return carry

    lax.fori_loop(0, BLK_DEV // 4, finish, 0)
    weight = acc[2 * FIELDS : 2 * FIELDS + 1]
    mass_total = jnp.broadcast_to(total[0:1, 127:128], (1, FOR_DEV))
    fmass[...] = weight * (FOR_DEV * PEERS / mass_total)
    fmean[...] = acc[:FIELDS] / weight
    fsecond[...] = acc[FIELDS : 2 * FIELDS] / weight


def pack(records, halo_mass, forest_id, dest_block, dest_slot):
    snaps, halos = halo_mass.shape
    groups = snaps * halos // 128
    by_group = records.reshape(FIELDS, snaps, halos // 128, 128).transpose(0, 2, 1, 3)
    by_group = by_group.reshape(FIELDS * groups, 128)
    vmem = pl.BlockSpec(memory_space=pltpu.VMEM)
    return pl.pallas_call(
        pack_kernel,
        out_shape=jax.ShapeDtypeStruct((PEERS, ROWS, 128), jnp.float32),
        in_specs=[pl.BlockSpec(memory_space=pl.ANY)] + [vmem] * 4,
        out_specs=vmem,
        scratch_shapes=[
            pltpu.VMEM((PEERS * CAP, 128), jnp.float32),
            pltpu.VMEM((FIELDS * groups, 128), jnp.float32),
            pltpu.VMEM((8 * groups, 128), jnp.float32),
            [pltpu.VMEM((128, 128), jnp.float32)] * 4,
            pltpu.VMEM((groups, 128), jnp.int32),
            [pltpu.SMEM((8, 128), jnp.int32)] * 2,
            pltpu.SemaphoreType.DMA,
            pltpu.SemaphoreType.DMA((2,)),
        ],
        compiler_params=pltpu.CompilerParams(vmem_limit_bytes=VMEM_LIMIT),
        name="pack",
    )(by_group, halo_mass, forest_id, dest_block, dest_slot)


def place(msg):
    f32 = jnp.float32
    vmem = pl.BlockSpec(memory_space=pltpu.VMEM)
    return pl.pallas_call(
        place_kernel,
        out_shape=(
            jax.ShapeDtypeStruct((FIELDS * BLK_DEV, 128), f32),
            jax.ShapeDtypeStruct((BLK_DEV, 128), f32),
            jax.ShapeDtypeStruct((1, FOR_DEV), f32),
            jax.ShapeDtypeStruct((FIELDS, FOR_DEV), f32),
            jax.ShapeDtypeStruct((FIELDS, FOR_DEV), f32),
        ),
        in_specs=[vmem],
        out_specs=(vmem,) * 5,
        scratch_shapes=[
            pltpu.VMEM((SLOTS + 8, 128), f32),
            pltpu.VMEM((2 * FIELDS + 8, FOR_DEV), f32),
            [pltpu.VMEM((CAP, 128), f32)] * 4,
            pltpu.VMEM((PEERS, 128), jnp.int32),
            [pltpu.SMEM((8, 128), jnp.int32)] * 2,
            pltpu.SemaphoreType.DMA((2,)),
        ],
        compiler_params=pltpu.CompilerParams(vmem_limit_bytes=VMEM_LIMIT),
        name="place",
    )(msg)


def on_device(records, halo_mass, forest_id, dest_block, dest_slot):
    outbox = pack(records, halo_mass, forest_id, dest_block, dest_slot)
    inbox = lax.all_to_all(outbox, EXCHANGE, split_axis=0, concat_axis=0, tiled=True)
    blocks, block_mass, fmass, fmean, fsecond = place(inbox)
    return blocks.reshape(FIELDS, BLK_DEV, 128), block_mass, fmass.reshape(FOR_DEV), fmean, fsecond


def solution(mesh):
    split = Mesh(
        mesh.devices.reshape(mesh.shape["row"], mesh.shape["sa"], 2, 2, 2, 2),
        ROW_SA_HA,
    )
    in_specs = (
        P(None, "sa", ROW_HA),
        P("sa", ROW_HA),
        P("sa", ROW_HA),
        P("sa", ROW_HA),
        P("sa", ROW_HA),
    )
    out_specs = (
        P(None, ROW_SA_HA, None),
        P(ROW_SA_HA, None),
        P(ROW_SA_HA),
        P(None, ROW_SA_HA),
        P(None, ROW_SA_HA),
    )
    return jax.shard_map(
        on_device, mesh=split, in_specs=in_specs, out_specs=out_specs, check_vma=False
    )
```

```python
import jax
import jax.numpy as jnp
from jax import lax
from jax.experimental import pallas as pl
from jax.experimental.pallas import tpu as pltpu
from jax.sharding import Mesh
from jax.sharding import PartitionSpec as P

FIELDS = 64
FOR_DEV = 128
BLK_DEV = 40
SLOTS = BLK_DEV * 128
PEERS = 64
CAP = 88
ROWS = 48
TAGS = 48
VMEM_LIMIT = 24 * 1024 * 1024
EXCHANGE = ("core", "sa", "z0", "z1", "z2")
ROW_HA = ("row", "z2", "z1", "z0", "core")
ROW_SA_HA = ("row", "sa", "z2", "z1", "z0", "core")


def iota(shape, dim):
    return lax.broadcasted_iota(jnp.int32, shape, dim)


def owner_of(block):
    return lax.shift_right_logical(block * 1639, 16)


def position_of(owner):
    core = (owner & 1) << 5
    plane = lax.shift_right_logical(owner, 4) << 3
    turned = ((owner & 2) << 1) | lax.shift_right_logical(owner & 4, 1) | lax.shift_right_logical(owner & 8, 3)
    return core | plane | turned


def rank_kernel(block, target, first_tag):
    groups = block.shape[0]
    before = (iota((256, 384), 0) < iota((256, 384), 1)) | (iota((256, 384), 1) >= 256)
    before = before.astype(jnp.float32).astype(jnp.bfloat16)
    peer = iota((PEERS, 128), 0)
    base = jnp.zeros((PEERS, 128), jnp.float32)
    goal = position_of(owner_of(block[...]))
    for g in range(0, groups, 2):
        member = jnp.concatenate([peer == goal[g : g + 1], peer == goal[g + 1 : g + 2]], axis=1)
        counts = jnp.dot(
            member.astype(jnp.float32).astype(jnp.bfloat16), before, preferred_element_type=jnp.float32
        )
        rank = counts[:, :256] + jnp.concatenate([base, base], axis=1)
        rank = jnp.sum(jnp.where(member, rank, 0.0), axis=0, keepdims=True).astype(jnp.int32)
        base = base + counts[:, 256:]
        first_tag[g : g + 1, :] = rank[:, :128]
        first_tag[g + 1 : g + 2, :] = rank[:, 128:]
    rank = first_tag[...]
    target[...] = goal * CAP + rank
    first_tag[...] = lax.shift_right_logical(rank, 3) << 2


def pack_kernel(
    target_v, first_tag, rec, mass, forest, block, slot_in, out, placed, slot, tiles, target_s, sems
):
    groups = mass.shape[0]

    def index_copy(k, buf):
        return pltpu.make_async_copy(
            target_v.at[pl.ds(pl.multiple_of(8 * k, 8), 8), :], target_s[buf], sems.at[buf]
        )

    index_copy(0, 0).start()
    index_copy(1, 1).start()
    for tile in tiles:
        tile[...] = jnp.zeros_like(tile)
    slot[...] = (block[...] - owner_of(block[...]) * BLK_DEV) * 128 + slot_in[...] + 1

    def clear(k, carry):
        placed[pl.ds(pl.multiple_of(k * 128, 128), 128), :] = jnp.zeros((128, 128), jnp.float32)
        return carry

    lax.fori_loop(0, PEERS * CAP // 128, clear, 0)
    line = iota((TAGS, 128), 0)

    def turn(group, tile):
        def row(ref):
            return jnp.broadcast_to(ref[pl.ds(group, 1), :], (TAGS, 128))

        own_line = line - row(first_tag)
        tags = jnp.where(own_line == 0, row(mass), 0.0)
        tags = jnp.where(own_line == 1, row(slot).astype(jnp.float32), tags)
        tags = jnp.where(own_line == 2, (row(forest) & (FOR_DEV - 1)).astype(jnp.float32), tags)
        stack = jnp.concatenate([rec[pl.ds(group, FIELDS, stride=groups), :], tags], axis=0)
        tile[:, : FIELDS + TAGS] = stack.T

    turn(0, tiles[0])

    def step(k, carry):
        for i in range(16):
            if i % 8 == 0:
                index_copy(0, i // 8).wait()
            after = jnp.minimum(16 * k + i + 1, groups - 1)
            turn(after, tiles[(i + 1) % 4])
            tile = tiles[i % 4]
            for r in range(128):
                placed[pl.ds(target_s[i // 8][i % 8, r], 1), :] = tile[r : r + 1, :]
            if i % 8 == 7:

                @pl.when(2 * k + i // 8 + 2 < groups // 8)
                def _():
                    index_copy(2 * k + i // 8 + 2, i // 8).start()

        return carry

    lax.fori_loop(0, groups // 16, step, 0)

    lane = iota((8, 128), 1)
    low = lane < FIELDS
    total = jnp.sum(jnp.sum(mass[...], axis=0, keepdims=True), axis=1, keepdims=True)
    corner = jnp.where(lane == 127, jnp.broadcast_to(total, (8, 128)), 0.0)

    def squeeze(k, carry):
        for h in range(8):
            p = 8 * k + h
            start = p * CAP
            rows = [placed[pl.ds(pl.multiple_of(start + 8 * v, 8), 8), :] for v in range(CAP // 8)]
            for v in range(5):
                out[p, 8 * v : 8 * v + 8, :] = jnp.where(low, rows[v], pltpu.roll(rows[v + 6], 64, 1))
            tags = corner
            for row in rows:
                tags = tags + row
            out[p, 40:48, :] = jnp.where(low, rows[5], tags)
        return carry

    lax.fori_loop(0, PEERS // 8, squeeze, 0)


def place_kernel(
    msg, blocks_hbm, block_mass, fmass, fmean, fsecond, blocks, placed, acc, tiles, slot_v, slot_s, sems, out_sems
):
    by_row = blocks.reshape(FIELDS * BLK_DEV, 128)
    lane = iota((8, 128), 1)
    low = lane < FIELDS
    slot_lane = (lane >= FIELDS) & (lane < FIELDS + 4 * (CAP // 8)) & (lane % 4 == 1)
    total = jnp.zeros((8, 128), jnp.float32)
    for g in range(PEERS // 8):
        index = jnp.zeros((8, 128), jnp.float32)
        for k in range(8):
            tags = msg[8 * g + k, 40:48, :]
            total = total + tags
            index = index + pltpu.roll(
                jnp.where(slot_lane, tags, 0.0), (64 * (k // 4) + k % 4 - 65) % 128, 1
            )
        index = index.astype(jnp.int32)
        slot_v[8 * g : 8 * g + 8, :] = jnp.where(index == 0, SLOTS, index - 1)

    def index_copy(g, buf):
        return pltpu.make_async_copy(
            slot_v.at[pl.ds(pl.multiple_of(8 * g, 8), 8), :], slot_s[buf], sems.at[buf]
        )

    index_copy(0, 0).start()
    index_copy(1, 1).start()

    def clear(k, carry):
        placed[pl.ds(pl.multiple_of(k * 128, 128), 128), :] = jnp.zeros((128, 128), jnp.float32)
        return carry

    lax.fori_loop(0, SLOTS // 128, clear, 0)
    acc[...] = jnp.zeros_like(acc)

    def turn(p, tile):
        tags = msg[p, 40:48, :]
        for v in range(CAP // 8):
            if v < 6:
                own = msg[p, 8 * v : 8 * v + 8, :]
            else:
                own = pltpu.roll(msg[p, 8 * v - 48 : 8 * v - 40, :], 64, 1)
            side = pltpu.roll(tags, 128 - 4 * v, 1) if v else tags
            tile[8 * v : 8 * v + 8, :] = jnp.where(low, own, side)

    turn(0, tiles[0])

    def step(k, carry):
        for i in range(16):
            if i % 8 == 0:
                index_copy(0, i // 8).wait()
            turn(jnp.minimum(16 * k + i + 1, PEERS - 1), tiles[(i + 1) % 4])
            tile = tiles[i % 4]
            for r in range(CAP):
                col = r // 8 * 4 + i % 8 % 4 + i % 8 // 4 * 64
                placed[pl.ds(slot_s[i // 8][r % 8, col], 1), :] = tile[r : r + 1, :]
            if i % 8 == 7:

                @pl.when(2 * k + i // 8 + 2 < PEERS // 8)
                def _():
                    index_copy(2 * k + i // 8 + 2, i // 8).start()

        return carry

    lax.fori_loop(0, PEERS // 16, step, 0)

    owned = iota((FOR_DEV, 128), 0)

    def out_copy(k):
        part = pl.ds(8 * k if isinstance(k, int) else pl.multiple_of(8 * k, 8), 8)
        return pltpu.make_async_copy(blocks.at[:, part, :], blocks_hbm.at[:, part, :], out_sems.at[k])

    def finish(k, carry):
        highs, lows, members = [], [], []
        for h in range(8):
            b = 8 * k + h
            view = placed[pl.ds(pl.multiple_of(b * 128, 128), 128), :].T
            x = view[:FIELDS]
            m = view[FIELDS : FIELDS + 1]
            by_row[pl.ds(b, FIELDS, stride=BLK_DEV), :] = x
            block_mass[pl.ds(b, 1), :] = m
            forest = view[FIELDS + 2 : FIELDS + 3].astype(jnp.int32)
            members.append((owned == forest).astype(jnp.float32).astype(jnp.bfloat16))
            scaled = m * x
            terms = jnp.concatenate([scaled, scaled * x, jnp.broadcast_to(m, (8, 128))], axis=0)
            high = terms.astype(jnp.bfloat16)
            highs.append(high)
            lows.append((terms - high.astype(jnp.float32)).astype(jnp.bfloat16))
        out_copy(k).start()
        member = jnp.concatenate(members, axis=1)
        for part in (highs, lows):
            acc[...] += lax.dot_general(
                jnp.concatenate(part, axis=1),
                member,
                (((1,), (1,)), ((), ())),
                preferred_element_type=jnp.float32,
            )
        return carry

    lax.fori_loop(0, BLK_DEV // 8, finish, 0)
    weight = acc[2 * FIELDS : 2 * FIELDS + 1]
    mass_total = jnp.broadcast_to(total[0:1, 127:128], (1, FOR_DEV))
    fmass[...] = weight * (FOR_DEV * PEERS / mass_total)
    fmean[...] = acc[:FIELDS] / weight
    fsecond[...] = acc[FIELDS : 2 * FIELDS] / weight
    for k in range(BLK_DEV // 8):
        out_copy(k).wait()


def pack(records, halo_mass, forest_id, dest_block, dest_slot):
    snaps, halos = halo_mass.shape
    groups = snaps * halos // 128

    def by_group(a):
        lead = a.shape[:-2]
        a = a.reshape(lead + (snaps, halos // 128, 128))
        return jnp.swapaxes(a, -3, -2).reshape(-1, 128)

    records, mass, forest, block, slot = map(by_group, (records, halo_mass, forest_id, dest_block, dest_slot))
    row = (groups, 128)
    vmem = pl.BlockSpec(memory_space=pltpu.VMEM)
    params = pltpu.CompilerParams(vmem_limit_bytes=VMEM_LIMIT)
    target, first_tag = pl.pallas_call(
        rank_kernel,
        out_shape=(jax.ShapeDtypeStruct(row, jnp.int32),) * 2,
        in_specs=[vmem],
        out_specs=(vmem,) * 2,
        cost_estimate=pl.CostEstimate(flops=2**31, bytes_accessed=2**16, transcendentals=0),
        compiler_params=params,
        name="rank",
    )(block)
    return pl.pallas_call(
        pack_kernel,
        out_shape=jax.ShapeDtypeStruct((PEERS, ROWS, 128), jnp.float32),
        in_specs=[vmem] * 7,
        out_specs=vmem,
        scratch_shapes=[
            pltpu.VMEM((PEERS * CAP, 128), jnp.float32),
            pltpu.VMEM(row, jnp.int32),
            [pltpu.VMEM((128, 128), jnp.float32)] * 4,
            [pltpu.SMEM((8, 128), jnp.int32)] * 2,
            pltpu.SemaphoreType.DMA((2,)),
        ],
        compiler_params=params,
        name="pack",
    )(target, first_tag, records, mass, forest, block, slot)


def place(msg):
    f32 = jnp.float32
    vmem = pl.BlockSpec(memory_space=pltpu.VMEM)
    return pl.pallas_call(
        place_kernel,
        out_shape=(
            jax.ShapeDtypeStruct((FIELDS, BLK_DEV, 128), f32),
            jax.ShapeDtypeStruct((BLK_DEV, 128), f32),
            jax.ShapeDtypeStruct((1, FOR_DEV), f32),
            jax.ShapeDtypeStruct((FIELDS, FOR_DEV), f32),
            jax.ShapeDtypeStruct((FIELDS, FOR_DEV), f32),
        ),
        in_specs=[vmem],
        out_specs=(pl.BlockSpec(memory_space=pltpu.HBM),) + (vmem,) * 4,
        scratch_shapes=[
            pltpu.VMEM((FIELDS, BLK_DEV, 128), f32),
            pltpu.VMEM((SLOTS + 8, 128), f32),
            pltpu.VMEM((2 * FIELDS + 8, FOR_DEV), f32),
            [pltpu.VMEM((CAP, 128), f32)] * 4,
            pltpu.VMEM((PEERS, 128), jnp.int32),
            [pltpu.SMEM((8, 128), jnp.int32)] * 2,
            pltpu.SemaphoreType.DMA((2,)),
            pltpu.SemaphoreType.DMA((BLK_DEV // 8,)),
        ],
        compiler_params=pltpu.CompilerParams(vmem_limit_bytes=VMEM_LIMIT),
        name="place",
    )(msg)


def on_device(records, halo_mass, forest_id, dest_block, dest_slot):
    outbox = pack(records, halo_mass, forest_id, dest_block, dest_slot)
    inbox = lax.all_to_all(outbox, EXCHANGE, split_axis=0, concat_axis=0, tiled=True)
    blocks, block_mass, fmass, fmean, fsecond = place(inbox)
    return blocks, block_mass, fmass.reshape(FOR_DEV), fmean, fsecond


def solution(mesh):
    split = Mesh(
        mesh.devices.reshape(mesh.shape["row"], mesh.shape["sa"], 2, 2, 2, 2),
        ROW_SA_HA,
    )
    in_specs = (
        P(None, "sa", ROW_HA),
        P("sa", ROW_HA),
        P("sa", ROW_HA),
        P("sa", ROW_HA),
        P("sa", ROW_HA),
    )
    out_specs = (
        P(None, ROW_SA_HA, None),
        P(ROW_SA_HA, None),
        P(ROW_SA_HA),
        P(None, ROW_SA_HA),
        P(None, ROW_SA_HA),
    )
    return jax.shard_map(
        on_device, mesh=split, in_specs=in_specs, out_specs=out_specs, check_vma=False
    )
```

```python
import jax
import jax.numpy as jnp
from jax import lax
from jax.experimental import pallas as pl
from jax.experimental.pallas import tpu as pltpu
from jax.sharding import Mesh
from jax.sharding import PartitionSpec as P

FIELDS = 64
FOR_DEV = 128
BLK_DEV = 40
SLOTS = BLK_DEV * 128
PEERS = 64
CAP = 88
ROWS = 48
TAGS = 48
PITCH = 40
VMEM_LIMIT = 24 * 1024 * 1024
EXCHANGE = ("core", "sa", "z0", "z1", "z2")
ROW_HA = ("row", "z2", "z1", "z0", "core")
ROW_SA_HA = ("row", "sa", "z2", "z1", "z0", "core")


def iota(shape, dim):
    return lax.broadcasted_iota(jnp.int32, shape, dim)


def owner_of(block):
    return lax.shift_right_logical(block * 1639, 16)


def position_of(owner):
    core = (owner & 1) << 5
    plane = lax.shift_right_logical(owner, 4) << 3
    turned = ((owner & 2) << 1) | lax.shift_right_logical(owner & 4, 1) | lax.shift_right_logical(owner & 8, 3)
    return core | plane | turned


def init_kernel(before, outbox, slots):
    ordered = (iota((256, 384), 0) < iota((256, 384), 1)) | (iota((256, 384), 1) >= 256)
    before[...] = ordered.astype(jnp.float32).astype(jnp.bfloat16)

    for array in (outbox, slots):

        def clear(k, carry):
            array[pl.ds(pl.multiple_of(k * 128, 128), 128), :] = jnp.zeros((128, 128), jnp.float32)
            return carry

        lax.fori_loop(0, array.shape[0] // 128, clear, 0)


def rank_kernel(block, before, target, first_tag):
    groups = block.shape[0]
    peer = iota((PEERS, 128), 0)
    base = jnp.zeros((PEERS, 128), jnp.float32)
    goal = position_of(owner_of(block[...]))
    for g in range(0, groups, 2):
        member = jnp.concatenate([peer == goal[g : g + 1], peer == goal[g + 1 : g + 2]], axis=1)
        counts = jnp.dot(
            member.astype(jnp.float32).astype(jnp.bfloat16), before[...], preferred_element_type=jnp.float32
        )
        rank = counts[:, :256] + jnp.concatenate([base, base], axis=1)
        rank = jnp.sum(jnp.where(member, rank, 0.0), axis=0, keepdims=True).astype(jnp.int32)
        base = base + counts[:, 256:]
        first_tag[g : g + 1, :] = rank[:, :128]
        first_tag[g + 1 : g + 2, :] = rank[:, 128:]
    rank = first_tag[...]
    target[...] = goal * CAP + rank
    first_tag[...] = lax.shift_right_logical(rank, 3) << 2


def pack_kernel(
    target_v, first_tag, rec, mass, forest, block, slot_in, start, out, placed, slot, spaced, tiles, target_s, sems
):
    del start
    groups = mass.shape[0]

    def index_copy(k, buf):
        return pltpu.make_async_copy(
            target_v.at[pl.ds(pl.multiple_of(8 * k, 8), 8), :], target_s[buf], sems.at[buf]
        )

    index_copy(0, 0).start()
    index_copy(1, 1).start()
    for tile in tiles:
        tile[...] = jnp.zeros_like(tile)
    slot[...] = (block[...] - owner_of(block[...]) * BLK_DEV) * 128 + slot_in[...] + 1

    for f in range(FIELDS):
        spaced[PITCH * f : PITCH * f + groups, :] = rec[groups * f : groups * f + groups, :]
    line = iota((TAGS, 128), 0)

    def turn(group, tile):
        def row(ref):
            return jnp.broadcast_to(ref[pl.ds(group, 1), :], (TAGS, 128))

        own_line = line - row(first_tag)
        tags = jnp.where(own_line == 0, row(mass), 0.0)
        tags = jnp.where(own_line == 1, row(slot).astype(jnp.float32), tags)
        tags = jnp.where(own_line == 2, (row(forest) & (FOR_DEV - 1)).astype(jnp.float32), tags)
        stack = jnp.concatenate([spaced[pl.ds(group, FIELDS, stride=PITCH), :], tags], axis=0)
        tile[:, : FIELDS + TAGS] = stack.T

    turn(0, tiles[0])

    def step(k, carry):
        for i in range(16):
            if i % 8 == 0:
                index_copy(0, i // 8).wait()
            after = jnp.minimum(16 * k + i + 1, groups - 1)
            turn(after, tiles[(i + 1) % 4])
            tile = tiles[i % 4]
            for r in range(128):
                placed[pl.ds(target_s[i // 8][i % 8, r], 1), :] = tile[r : r + 1, :]
            if i % 8 == 7:
                index_copy(jnp.minimum(2 * k + i // 8 + 2, groups // 8 - 1), i // 8).start()
        return carry

    lax.fori_loop(0, groups // 16, step, 0)
    for buf in range(2):
        index_copy(0, buf).wait()

    lane = iota((8, 128), 1)
    low = lane < FIELDS
    total = jnp.sum(jnp.sum(mass[...], axis=0, keepdims=True), axis=1, keepdims=True)
    corner = jnp.where(lane == 127, jnp.broadcast_to(total, (8, 128)), 0.0)

    def squeeze(k, carry):
        for h in range(8):
            p = 8 * k + h
            start = p * CAP
            rows = [placed[pl.ds(pl.multiple_of(start + 8 * v, 8), 8), :] for v in range(CAP // 8)]
            for v in range(5):
                out[p, 8 * v : 8 * v + 8, :] = jnp.where(low, rows[v], pltpu.roll(rows[v + 6], 64, 1))
            tags = corner
            for row in rows:
                tags = tags + row
            out[p, 40:48, :] = jnp.where(low, rows[5], tags)
        return carry

    lax.fori_loop(0, PEERS // 8, squeeze, 0)


def place_kernel(
    msg, start, blocks_hbm, block_mass_hbm, fmass_hbm, fmean_hbm, fsecond_hbm, placed,
    blocks, block_mass, fmass, fmean, fsecond, acc, tiles, slot_v, slot_s, sems, out_sems,
):
    del start
    by_row = blocks.reshape(FIELDS * BLK_DEV, 128)

    def index_copy(g, buf):
        return pltpu.make_async_copy(
            slot_v.at[pl.ds(pl.multiple_of(8 * g, 8), 8), :], slot_s[buf], sems.at[buf]
        )

    lane = iota((8, 128), 1)
    low = lane < FIELDS
    slot_lane = (lane >= FIELDS) & (lane < FIELDS + 4 * (CAP // 8)) & (lane % 4 == 1)
    total = jnp.zeros((8, 128), jnp.float32)
    for g in range(PEERS // 8):
        index = jnp.zeros((8, 128), jnp.float32)
        for k in range(8):
            tags = msg[8 * g + k, 40:48, :]
            total = total + tags
            index = index + pltpu.roll(
                jnp.where(slot_lane, tags, 0.0), (64 * (k // 4) + k % 4 - 65) % 128, 1
            )
        index = index.astype(jnp.int32)
        slot_v[8 * g : 8 * g + 8, :] = jnp.where(index == 0, SLOTS, index - 1)
        if g < 2:
            index_copy(g, g).start()
    acc[...] = jnp.zeros_like(acc)

    def turn(p, tile):
        tags = msg[p, 40:48, :]
        for v in range(CAP // 8):
            if v < 6:
                own = msg[p, 8 * v : 8 * v + 8, :]
            else:
                own = pltpu.roll(msg[p, 8 * v - 48 : 8 * v - 40, :], 64, 1)
            side = pltpu.roll(tags, 128 - 4 * v, 1) if v else tags
            tile[8 * v : 8 * v + 8, :] = jnp.where(low, own, side)

    turn(0, tiles[0])

    def step(k, carry):
        for i in range(16):
            if i % 8 == 0:
                index_copy(0, i // 8).wait()
            turn(jnp.minimum(16 * k + i + 1, PEERS - 1), tiles[(i + 1) % 4])
            tile = tiles[i % 4]
            for r in range(CAP):
                col = r // 8 * 4 + i % 8 % 4 + i % 8 // 4 * 64
                placed[pl.ds(slot_s[i // 8][r % 8, col], 1), :] = tile[r : r + 1, :]
            if i % 8 == 7:
                index_copy(jnp.minimum(2 * k + i // 8 + 2, PEERS // 8 - 1), i // 8).start()
        return carry

    lax.fori_loop(0, PEERS // 16, step, 0)
    for buf in range(2):
        index_copy(0, buf).wait()

    owned = iota((FOR_DEV, 128), 0)

    def out_copy(k):
        part = pl.ds(8 * k if isinstance(k, int) else pl.multiple_of(8 * k, 8), 8)
        return pltpu.make_async_copy(blocks.at[:, part, :], blocks_hbm.at[:, part, :], out_sems.at[k])

    def finish(k, carry):
        highs, lows, members = [], [], []
        for h in range(8):
            b = 8 * k + h
            view = placed[pl.ds(pl.multiple_of(b * 128, 128), 128), :].T
            x = view[:FIELDS]
            m = view[FIELDS : FIELDS + 1]
            by_row[pl.ds(b, FIELDS, stride=BLK_DEV), :] = x
            block_mass[pl.ds(b, 1), :] = m
            forest = view[FIELDS + 2 : FIELDS + 3].astype(jnp.int32)
            members.append((owned == forest).astype(jnp.float32).astype(jnp.bfloat16))
            scaled = m * x
            terms = jnp.concatenate([scaled, scaled * x, jnp.broadcast_to(m, (8, 128))], axis=0)
            high = terms.astype(jnp.bfloat16)
            highs.append(high)
            lows.append((terms - high.astype(jnp.float32)).astype(jnp.bfloat16))
        out_copy(k).start()
        member = jnp.concatenate(members, axis=1)
        for part in (highs, lows):
            acc[...] += lax.dot_general(
                jnp.concatenate(part, axis=1),
                member,
                (((1,), (1,)), ((), ())),
                preferred_element_type=jnp.float32,
            )
        return carry

    lax.fori_loop(0, BLK_DEV // 8, finish, 0)
    others = [
        pltpu.make_async_copy(src, dst, out_sems.at[BLK_DEV // 8 + n])
        for n, (src, dst) in enumerate(
            ((block_mass, block_mass_hbm), (fmass, fmass_hbm), (fmean, fmean_hbm), (fsecond, fsecond_hbm))
        )
    ]
    others[0].start()
    weight = acc[2 * FIELDS : 2 * FIELDS + 1]
    mass_total = jnp.broadcast_to(total[0:1, 127:128], (1, FOR_DEV))
    fmass[...] = weight * (FOR_DEV * PEERS / mass_total)
    others[1].start()
    fmean[...] = acc[:FIELDS] / weight
    others[2].start()
    fsecond[...] = acc[FIELDS : 2 * FIELDS] / weight
    others[3].start()
    for copy in [out_copy(k) for k in range(BLK_DEV // 8)] + others:
        copy.wait()


def pack(records, halo_mass, forest_id, dest_block, dest_slot):
    snaps, halos = halo_mass.shape
    groups = snaps * halos // 128

    def by_group(a):
        lead = a.shape[:-2]
        a = a.reshape(lead + (snaps, halos // 128, 128))
        return jnp.swapaxes(a, -3, -2).reshape(-1, 128)

    records, mass, forest, block, slot = map(by_group, (records, halo_mass, forest_id, dest_block, dest_slot))
    row = (groups, 128)
    vmem = pl.BlockSpec(memory_space=pltpu.VMEM)
    params = pltpu.CompilerParams(vmem_limit_bytes=VMEM_LIMIT)
    before, placed, slots = pl.pallas_call(
        init_kernel,
        out_shape=(
            jax.ShapeDtypeStruct((256, 384), jnp.bfloat16),
            jax.ShapeDtypeStruct((PEERS * CAP, 128), jnp.float32),
            jax.ShapeDtypeStruct((SLOTS + 128, 128), jnp.float32),
        ),
        out_specs=(vmem,) * 3,
        cost_estimate=pl.CostEstimate(flops=2**31, bytes_accessed=2**16, transcendentals=0),
        compiler_params=params,
        name="init",
    )()
    target, first_tag = pl.pallas_call(
        rank_kernel,
        out_shape=(jax.ShapeDtypeStruct(row, jnp.int32),) * 2,
        in_specs=[vmem] * 2,
        out_specs=(vmem,) * 2,
        cost_estimate=pl.CostEstimate(flops=2**20, bytes_accessed=2**16, transcendentals=0),
        compiler_params=params,
        name="rank",
    )(block, before)
    outbox, _ = pl.pallas_call(
        pack_kernel,
        out_shape=(
            jax.ShapeDtypeStruct((PEERS, ROWS, 128), jnp.float32),
            jax.ShapeDtypeStruct((PEERS * CAP, 128), jnp.float32),
        ),
        in_specs=[vmem] * 8,
        out_specs=(vmem, pl.BlockSpec(memory_space=pltpu.VMEM)),
        input_output_aliases={7: 1},
        scratch_shapes=[
            pltpu.VMEM(row, jnp.int32),
            pltpu.VMEM((FIELDS * PITCH, 128), jnp.float32),
            [pltpu.VMEM((128, 128), jnp.float32)] * 4,
            [pltpu.SMEM((8, 128), jnp.int32)] * 2,
            pltpu.SemaphoreType.DMA((2,)),
        ],
        compiler_params=params,
        name="pack",
    )(target, first_tag, records, mass, forest, block, slot, placed)
    return outbox, slots


def place(msg, slots):
    f32 = jnp.float32
    vmem = pl.BlockSpec(memory_space=pltpu.VMEM)
    shapes = ((FIELDS, BLK_DEV, 128), (BLK_DEV, 128), (1, FOR_DEV), (FIELDS, FOR_DEV), (FIELDS, FOR_DEV))
    return pl.pallas_call(
        place_kernel,
        out_shape=tuple(jax.ShapeDtypeStruct(shape, f32) for shape in shapes + (slots.shape,)),
        in_specs=[vmem] * 2,
        out_specs=(pl.BlockSpec(memory_space=pltpu.HBM),) * 5 + (vmem,),
        input_output_aliases={1: 5},
        scratch_shapes=[pltpu.VMEM(shape, f32) for shape in shapes]
        + [
            pltpu.VMEM((2 * FIELDS + 8, FOR_DEV), f32),
            [pltpu.VMEM((CAP, 128), f32)] * 4,
            pltpu.VMEM((PEERS, 128), jnp.int32),
            [pltpu.SMEM((8, 128), jnp.int32)] * 2,
            pltpu.SemaphoreType.DMA((2,)),
            pltpu.SemaphoreType.DMA((BLK_DEV // 8 + 4,)),
        ],
        compiler_params=pltpu.CompilerParams(vmem_limit_bytes=VMEM_LIMIT),
        name="place",
    )(msg, slots)[:5]


def on_device(records, halo_mass, forest_id, dest_block, dest_slot):
    outbox, slots = pack(records, halo_mass, forest_id, dest_block, dest_slot)
    inbox = lax.all_to_all(outbox, EXCHANGE, split_axis=0, concat_axis=0, tiled=True)
    blocks, block_mass, fmass, fmean, fsecond = place(inbox, slots)
    return blocks, block_mass, fmass.reshape(FOR_DEV), fmean, fsecond


def solution(mesh):
    split = Mesh(
        mesh.devices.reshape(mesh.shape["row"], mesh.shape["sa"], 2, 2, 2, 2),
        ROW_SA_HA,
    )
    in_specs = (
        P(None, "sa", ROW_HA),
        P("sa", ROW_HA),
        P("sa", ROW_HA),
        P("sa", ROW_HA),
        P("sa", ROW_HA),
    )
    out_specs = (
        P(None, ROW_SA_HA, None),
        P(ROW_SA_HA, None),
        P(ROW_SA_HA),
        P(None, ROW_SA_HA),
        P(None, ROW_SA_HA),
    )
    return jax.shard_map(
        on_device, mesh=split, in_specs=in_specs, out_specs=out_specs, check_vma=False
    )
```

```python
import jax
import jax.numpy as jnp
from jax import lax
from jax.experimental import pallas as pl
from jax.experimental.pallas import tpu as pltpu
from jax.sharding import Mesh
from jax.sharding import PartitionSpec as P

FIELDS = 64
FOR_DEV = 128
BLK_DEV = 40
SLOTS = BLK_DEV * 128
PEERS = 64
CAP = 88
ROWS = 48
TAGS = 48
PITCH = 40
VMEM_LIMIT = 24 * 1024 * 1024
EXCHANGE = ("core", "sa", "z0", "z1", "z2")
ROW_HA = ("row", "z2", "z1", "z0", "core")
ROW_SA_HA = ("row", "sa", "z2", "z1", "z0", "core")


def iota(shape, dim):
    return lax.broadcasted_iota(jnp.int32, shape, dim)


def owner_of(block):
    return lax.shift_right_logical(block * 1639, 16)


def position_of(owner):
    core = (owner & 1) << 5
    plane = lax.shift_right_logical(owner, 4) << 3
    turned = ((owner & 2) << 1) | lax.shift_right_logical(owner & 4, 1) | lax.shift_right_logical(owner & 8, 3)
    return core | plane | turned


def init_kernel(before, outbox, slots):
    ordered = (iota((256, 384), 0) < iota((256, 384), 1)) | (iota((256, 384), 1) >= 256)
    before[...] = ordered.astype(jnp.float32).astype(jnp.bfloat16)

    for array in (outbox, slots):

        def clear(k, carry):
            array[pl.ds(pl.multiple_of(k * 128, 128), 128), :] = jnp.zeros((128, 128), jnp.float32)
            return carry

        lax.fori_loop(0, array.shape[0] // 128, clear, 0)


def rank_kernel(block, before, target, first_tag):
    groups = block.shape[0]
    peer = iota((PEERS, 128), 0)
    base = jnp.zeros((PEERS, 128), jnp.float32)
    goal = position_of(owner_of(block[...]))
    for g in range(0, groups, 2):
        member = jnp.concatenate([peer == goal[g : g + 1], peer == goal[g + 1 : g + 2]], axis=1)
        counts = jnp.dot(
            member.astype(jnp.float32).astype(jnp.bfloat16), before[...], preferred_element_type=jnp.float32
        )
        rank = counts[:, :256] + jnp.concatenate([base, base], axis=1)
        rank = jnp.sum(jnp.where(member, rank, 0.0), axis=0, keepdims=True).astype(jnp.int32)
        base = base + counts[:, 256:]
        first_tag[g : g + 1, :] = rank[:, :128]
        first_tag[g + 1 : g + 2, :] = rank[:, 128:]
    rank = first_tag[...]
    target[...] = goal * CAP + rank
    first_tag[...] = lax.shift_right_logical(rank, 3) << 2


def pack_kernel(
    target_v, first_tag, rec, mass, forest, block, slot_in, start, out, placed, slot, spaced, tiles, target_s, sems
):
    del start
    groups = mass.shape[0]

    def index_copy(k):
        return pltpu.make_async_copy(target_v.at[8 * k : 8 * k + 8, :], target_s[k], sems.at[k])

    for k in range(groups // 8):
        index_copy(k).start()
    for tile in tiles:
        tile[...] = jnp.zeros_like(tile)
    slot[...] = (block[...] - owner_of(block[...]) * BLK_DEV) * 128 + slot_in[...] + 1

    for f in range(FIELDS):
        spaced[PITCH * f : PITCH * f + groups, :] = rec[groups * f : groups * f + groups, :]
    line = iota((TAGS, 128), 0)

    def turn(group, tile):
        def row(ref):
            return jnp.broadcast_to(ref[pl.ds(group, 1), :], (TAGS, 128))

        own_line = line - row(first_tag)
        tags = jnp.where(own_line == 0, row(mass), 0.0)
        tags = jnp.where(own_line == 1, row(slot).astype(jnp.float32), tags)
        tags = jnp.where(own_line == 2, (row(forest) & (FOR_DEV - 1)).astype(jnp.float32), tags)
        stack = jnp.concatenate([spaced[pl.ds(group, FIELDS, stride=PITCH), :], tags], axis=0)
        tile[:, : FIELDS + TAGS] = stack.T

    turn(0, tiles[0])

    for i in range(groups):
        if i % 8 == 0:
            index_copy(i // 8).wait()
        if i + 1 < groups:
            turn(i + 1, tiles[(i + 1) % 4])
        tile = tiles[i % 4]
        for r in range(128):
            placed[pl.ds(target_s[i // 8][i % 8, r], 1), :] = tile[r : r + 1, :]

    lane = iota((8, 128), 1)
    low = lane < FIELDS
    total = jnp.sum(jnp.sum(mass[...], axis=0, keepdims=True), axis=1, keepdims=True)
    corner = jnp.where(lane == 127, jnp.broadcast_to(total, (8, 128)), 0.0)

    def squeeze(k, carry):
        for h in range(8):
            p = 8 * k + h
            start = p * CAP
            rows = [placed[pl.ds(pl.multiple_of(start + 8 * v, 8), 8), :] for v in range(CAP // 8)]
            for v in range(5):
                out[p, 8 * v : 8 * v + 8, :] = jnp.where(low, rows[v], pltpu.roll(rows[v + 6], 64, 1))
            tags = corner
            for row in rows:
                tags = tags + row
            out[p, 40:48, :] = jnp.where(low, rows[5], tags)
        return carry

    lax.fori_loop(0, PEERS // 8, squeeze, 0)


def place_kernel(
    msg, start, blocks_hbm, block_mass_hbm, fmass_hbm, fmean_hbm, fsecond_hbm, placed,
    blocks, block_mass, fmass, fmean, fsecond, acc, tiles, slot_v, slot_s, sems, out_sems,
):
    del start
    by_row = blocks.reshape(FIELDS * BLK_DEV, 128)

    def index_copy(g, buf):
        return pltpu.make_async_copy(
            slot_v.at[pl.ds(pl.multiple_of(8 * g, 8), 8), :], slot_s[buf], sems.at[buf]
        )

    lane = iota((8, 128), 1)
    low = lane < FIELDS
    slot_lane = (lane >= FIELDS) & (lane < FIELDS + 4 * (CAP // 8)) & (lane % 4 == 1)
    total = jnp.zeros((8, 128), jnp.float32)
    for g in range(PEERS // 8):
        index = jnp.zeros((8, 128), jnp.float32)
        for k in range(8):
            tags = msg[8 * g + k, 40:48, :]
            total = total + tags
            index = index + pltpu.roll(
                jnp.where(slot_lane, tags, 0.0), (64 * (k // 4) + k % 4 - 65) % 128, 1
            )
        index = index.astype(jnp.int32)
        slot_v[8 * g : 8 * g + 8, :] = jnp.where(index == 0, SLOTS, index - 1)
        if g < 4:
            index_copy(g, g).start()
    acc[...] = jnp.zeros_like(acc)

    def turn(p, tile):
        tags = msg[p, 40:48, :]
        for v in range(CAP // 8):
            if v < 6:
                own = msg[p, 8 * v : 8 * v + 8, :]
            else:
                own = pltpu.roll(msg[p, 8 * v - 48 : 8 * v - 40, :], 64, 1)
            side = pltpu.roll(tags, 128 - 4 * v, 1) if v else tags
            tile[8 * v : 8 * v + 8, :] = jnp.where(low, own, side)

    turn(0, tiles[0])

    def step(k, carry):
        for i in range(32):
            if i % 8 == 0:
                index_copy(0, i // 8).wait()
            turn(jnp.minimum(32 * k + i + 1, PEERS - 1), tiles[(i + 1) % 4])
            tile = tiles[i % 4]
            for r in range(CAP):
                col = r // 8 * 4 + i % 8 % 4 + i % 8 // 4 * 64
                placed[pl.ds(slot_s[i // 8][r % 8, col], 1), :] = tile[r : r + 1, :]
            if i % 8 == 7:
                index_copy(jnp.minimum(4 * k + i // 8 + 4, PEERS // 8 - 1), i // 8).start()

        return carry

    lax.fori_loop(0, PEERS // 32, step, 0)
    for buf in range(4):
        index_copy(0, buf).wait()

    owned = iota((FOR_DEV, 128), 0)

    def out_copy(k):
        part = pl.ds(8 * k if isinstance(k, int) else pl.multiple_of(8 * k, 8), 8)
        return pltpu.make_async_copy(blocks.at[:, part, :], blocks_hbm.at[:, part, :], out_sems.at[k])

    def finish(k, carry):
        highs, lows, members = [], [], []
        for h in range(8):
            b = 8 * k + h
            view = placed[pl.ds(pl.multiple_of(b * 128, 128), 128), :].T
            x = view[:FIELDS]
            m = view[FIELDS : FIELDS + 1]
            by_row[pl.ds(b, FIELDS, stride=BLK_DEV), :] = x
            block_mass[pl.ds(b, 1), :] = m
            forest = view[FIELDS + 2 : FIELDS + 3].astype(jnp.int32)
            members.append((owned == forest).astype(jnp.float32).astype(jnp.bfloat16))
            scaled = m * x
            terms = jnp.concatenate([scaled, scaled * x, jnp.broadcast_to(m, (8, 128))], axis=0)
            high = terms.astype(jnp.bfloat16)
            highs.append(high)
            lows.append((terms - high.astype(jnp.float32)).astype(jnp.bfloat16))
        out_copy(k).start()
        member = jnp.concatenate(members, axis=1)
        for part in (highs, lows):
            acc[...] += lax.dot_general(
                jnp.concatenate(part, axis=1),
                member,
                (((1,), (1,)), ((), ())),
                preferred_element_type=jnp.float32,
            )
        return carry

    lax.fori_loop(0, BLK_DEV // 8, finish, 0)
    others = [
        pltpu.make_async_copy(src, dst, out_sems.at[BLK_DEV // 8 + n])
        for n, (src, dst) in enumerate(
            ((block_mass, block_mass_hbm), (fmass, fmass_hbm), (fmean, fmean_hbm), (fsecond, fsecond_hbm))
        )
    ]
    others[0].start()
    weight = acc[2 * FIELDS : 2 * FIELDS + 1]
    mass_total = jnp.broadcast_to(total[0:1, 127:128], (1, FOR_DEV))
    fmass[...] = weight * (FOR_DEV * PEERS / mass_total)
    others[1].start()
    fmean[...] = acc[:FIELDS] / weight
    others[2].start()
    fsecond[...] = acc[FIELDS : 2 * FIELDS] / weight
    others[3].start()
    for copy in [out_copy(k) for k in range(BLK_DEV // 8)] + others:
        copy.wait()


def pack(records, halo_mass, forest_id, dest_block, dest_slot):
    snaps, halos = halo_mass.shape
    groups = snaps * halos // 128

    def by_group(a):
        lead = a.shape[:-2]
        a = a.reshape(lead + (snaps, halos // 128, 128))
        return jnp.swapaxes(a, -3, -2).reshape(-1, 128)

    records, mass, forest, block, slot = map(by_group, (records, halo_mass, forest_id, dest_block, dest_slot))
    row = (groups, 128)
    vmem = pl.BlockSpec(memory_space=pltpu.VMEM)
    params = pltpu.CompilerParams(vmem_limit_bytes=VMEM_LIMIT)
    before, placed, slots = pl.pallas_call(
        init_kernel,
        out_shape=(
            jax.ShapeDtypeStruct((256, 384), jnp.bfloat16),
            jax.ShapeDtypeStruct((PEERS * CAP, 128), jnp.float32),
            jax.ShapeDtypeStruct((SLOTS + 128, 128), jnp.float32),
        ),
        out_specs=(vmem,) * 3,
        cost_estimate=pl.CostEstimate(flops=2**31, bytes_accessed=2**16, transcendentals=0),
        compiler_params=params,
        name="init",
    )()
    target, first_tag = pl.pallas_call(
        rank_kernel,
        out_shape=(jax.ShapeDtypeStruct(row, jnp.int32),) * 2,
        in_specs=[vmem] * 2,
        out_specs=(vmem,) * 2,
        cost_estimate=pl.CostEstimate(flops=2**20, bytes_accessed=2**16, transcendentals=0),
        compiler_params=params,
        name="rank",
    )(block, before)
    outbox, _ = pl.pallas_call(
        pack_kernel,
        out_shape=(
            jax.ShapeDtypeStruct((PEERS, ROWS, 128), jnp.float32),
            jax.ShapeDtypeStruct((PEERS * CAP, 128), jnp.float32),
        ),
        in_specs=[vmem] * 8,
        out_specs=(vmem, pl.BlockSpec(memory_space=pltpu.VMEM)),
        input_output_aliases={7: 1},
        scratch_shapes=[
            pltpu.VMEM(row, jnp.int32),
            pltpu.VMEM((FIELDS * PITCH, 128), jnp.float32),
            [pltpu.VMEM((128, 128), jnp.float32)] * 4,
            [pltpu.SMEM((8, 128), jnp.int32)] * (groups // 8),
            pltpu.SemaphoreType.DMA((groups // 8,)),
        ],
        compiler_params=params,
        name="pack",
    )(target, first_tag, records, mass, forest, block, slot, placed)
    return outbox, slots


def place(msg, slots):
    f32 = jnp.float32
    vmem = pl.BlockSpec(memory_space=pltpu.VMEM)
    shapes = ((FIELDS, BLK_DEV, 128), (BLK_DEV, 128), (1, FOR_DEV), (FIELDS, FOR_DEV), (FIELDS, FOR_DEV))
    return pl.pallas_call(
        place_kernel,
        out_shape=tuple(jax.ShapeDtypeStruct(shape, f32) for shape in shapes + (slots.shape,)),
        in_specs=[vmem] * 2,
        out_specs=(pl.BlockSpec(memory_space=pltpu.HBM),) * 5 + (vmem,),
        input_output_aliases={1: 5},
        scratch_shapes=[pltpu.VMEM(shape, f32) for shape in shapes]
        + [
            pltpu.VMEM((2 * FIELDS + 8, FOR_DEV), f32),
            [pltpu.VMEM((CAP, 128), f32)] * 4,
            pltpu.VMEM((PEERS, 128), jnp.int32),
            [pltpu.SMEM((8, 128), jnp.int32)] * 4,
            pltpu.SemaphoreType.DMA((4,)),
            pltpu.SemaphoreType.DMA((BLK_DEV // 8 + 4,)),
        ],
        compiler_params=pltpu.CompilerParams(vmem_limit_bytes=VMEM_LIMIT),
        name="place",
    )(msg, slots)[:5]


def on_device(records, halo_mass, forest_id, dest_block, dest_slot):
    outbox, slots = pack(records, halo_mass, forest_id, dest_block, dest_slot)
    inbox = lax.all_to_all(outbox, EXCHANGE, split_axis=0, concat_axis=0, tiled=True)
    blocks, block_mass, fmass, fmean, fsecond = place(inbox, slots)
    return blocks, block_mass, fmass.reshape(FOR_DEV), fmean, fsecond


def solution(mesh):
    split = Mesh(
        mesh.devices.reshape(mesh.shape["row"], mesh.shape["sa"], 2, 2, 2, 2),
        ROW_SA_HA,
    )
    in_specs = (
        P(None, "sa", ROW_HA),
        P("sa", ROW_HA),
        P("sa", ROW_HA),
        P("sa", ROW_HA),
        P("sa", ROW_HA),
    )
    out_specs = (
        P(None, ROW_SA_HA, None),
        P(ROW_SA_HA, None),
        P(ROW_SA_HA),
        P(None, ROW_SA_HA),
        P(None, ROW_SA_HA),
    )
    return jax.shard_map(
        on_device, mesh=split, in_specs=in_specs, out_specs=out_specs, check_vma=False
    )
```

```python
import jax
import jax.numpy as jnp
from jax import lax
from jax.experimental import pallas as pl
from jax.experimental.pallas import tpu as pltpu
from jax.sharding import Mesh
from jax.sharding import PartitionSpec as P

FIELDS = 64
FOR_DEV = 128
BLK_DEV = 40
SLOTS = BLK_DEV * 128
PEERS = 64
CAP = 88
ROWS = 48
TAGS = 48
PITCH = 40
VMEM_LIMIT = 24 * 1024 * 1024
EXCHANGE = ("core", "sa", "z0", "z1", "z2")
ROW_HA = ("row", "z2", "z1", "z0", "core")
ROW_SA_HA = ("row", "sa", "z2", "z1", "z0", "core")


def iota(shape, dim):
    return lax.broadcasted_iota(jnp.int32, shape, dim)


def owner_of(block):
    return lax.shift_right_logical(block * 1639, 16)


def position_of(owner):
    core = (owner & 1) << 5
    plane = lax.shift_right_logical(owner, 4) << 3
    turned = ((owner & 2) << 1) | lax.shift_right_logical(owner & 4, 1) | lax.shift_right_logical(owner & 8, 3)
    return core | plane | turned


def init_kernel(before, outbox, slots):
    ordered = (iota((256, 384), 0) < iota((256, 384), 1)) | (iota((256, 384), 1) >= 256)
    before[...] = ordered.astype(jnp.float32).astype(jnp.bfloat16)

    for array in (outbox, slots):

        def clear(k, carry):
            array[pl.ds(pl.multiple_of(k * 128, 128), 128), :] = jnp.zeros((128, 128), jnp.float32)
            return carry

        lax.fori_loop(0, array.shape[0] // 128, clear, 0)


def rank_kernel(block, before, target, first_tag):
    groups = block.shape[0]
    peer = iota((PEERS, 128), 0)
    base = jnp.zeros((PEERS, 128), jnp.float32)
    goal = position_of(owner_of(block[...]))
    for g in range(0, groups, 2):
        member = jnp.concatenate([peer == goal[g : g + 1], peer == goal[g + 1 : g + 2]], axis=1)
        counts = jnp.dot(
            member.astype(jnp.float32).astype(jnp.bfloat16), before[...], preferred_element_type=jnp.float32
        )
        rank = counts[:, :256] + jnp.concatenate([base, base], axis=1)
        rank = jnp.sum(jnp.where(member, rank, 0.0), axis=0, keepdims=True).astype(jnp.int32)
        base = base + counts[:, 256:]
        first_tag[g : g + 1, :] = rank[:, :128]
        first_tag[g + 1 : g + 2, :] = rank[:, 128:]
    rank = first_tag[...]
    target[...] = goal * CAP + rank
    first_tag[...] = lax.shift_right_logical(rank, 3) << 2


def pack_kernel(
    target_v, first_tag, rec, mass, forest, block, slot_in, start, out, placed, slot, spaced, tiles, target_s, sems
):
    del start
    groups = mass.shape[0]

    def index_copy(k):
        return pltpu.make_async_copy(target_v.at[8 * k : 8 * k + 8, :], target_s[k], sems.at[k])

    for k in range(groups // 8):
        index_copy(k).start()
    for tile in tiles:
        tile[...] = jnp.zeros_like(tile)
    slot[...] = (block[...] - owner_of(block[...]) * BLK_DEV) * 128 + slot_in[...] + 1

    for f in range(FIELDS):
        spaced[PITCH * f : PITCH * f + groups, :] = rec[groups * f : groups * f + groups, :]
    line = iota((TAGS, 128), 0)

    def turn(group, tile):
        def row(ref):
            return jnp.broadcast_to(ref[pl.ds(group, 1), :], (TAGS, 128))

        own_line = line - row(first_tag)
        tags = jnp.where(own_line == 0, row(mass), 0.0)
        tags = jnp.where(own_line == 1, row(slot).astype(jnp.float32), tags)
        tags = jnp.where(own_line == 2, (row(forest) & (FOR_DEV - 1)).astype(jnp.float32), tags)
        stack = jnp.concatenate([spaced[pl.ds(group, FIELDS, stride=PITCH), :], tags], axis=0)
        tile[:, : FIELDS + TAGS] = stack.T

    turn(0, tiles[0])

    for i in range(groups):
        if i % 8 == 0:
            index_copy(i // 8).wait()
        if i + 1 < groups:
            turn(i + 1, tiles[(i + 1) % 4])
        tile = tiles[i % 4]
        for r in range(128):
            placed[pl.ds(target_s[i // 8][i % 8, r], 1), :] = tile[r : r + 1, :]

    lane = iota((8, 128), 1)
    low = lane < FIELDS
    total = jnp.sum(jnp.sum(mass[...], axis=0, keepdims=True), axis=1, keepdims=True)
    corner = jnp.where(lane == 127, jnp.broadcast_to(total, (8, 128)), 0.0)

    def squeeze(k, carry):
        for h in range(16):
            p = 16 * k + h
            start = p * CAP
            rows = [placed[pl.ds(pl.multiple_of(start + 8 * v, 8), 8), :] for v in range(CAP // 8)]
            for v in range(5):
                out[p, 8 * v : 8 * v + 8, :] = jnp.where(low, rows[v], pltpu.roll(rows[v + 6], 64, 1))
            tags = corner
            for row in rows:
                tags = tags + row
            out[p, 40:48, :] = jnp.where(low, rows[5], tags)
        return carry

    lax.fori_loop(0, PEERS // 16, squeeze, 0)


def place_kernel(
    msg, start, blocks_hbm, block_mass_hbm, fmass_hbm, fmean_hbm, fsecond_hbm, placed,
    blocks, block_mass, fmass, fmean, fsecond, acc, tiles, slot_v, slot_s, sems, out_sems,
):
    del start
    by_row = blocks.reshape(FIELDS * BLK_DEV, 128)

    def index_copy(g, buf):
        return pltpu.make_async_copy(
            slot_v.at[pl.ds(pl.multiple_of(8 * g, 8), 8), :], slot_s[buf], sems.at[buf]
        )

    lane = iota((8, 128), 1)
    low = lane < FIELDS
    slot_lane = (lane >= FIELDS) & (lane < FIELDS + 4 * (CAP // 8)) & (lane % 4 == 1)
    total = jnp.zeros((8, 128), jnp.float32)
    for g in range(PEERS // 8):
        index = jnp.zeros((8, 128), jnp.float32)
        for k in range(8):
            tags = msg[8 * g + k, 40:48, :]
            total = total + tags
            index = index + pltpu.roll(
                jnp.where(slot_lane, tags, 0.0), (64 * (k // 4) + k % 4 - 65) % 128, 1
            )
        index = index.astype(jnp.int32)
        slot_v[8 * g : 8 * g + 8, :] = jnp.where(index == 0, SLOTS, index - 1)
        if g < 4:
            index_copy(g, g).start()
    acc[...] = jnp.zeros_like(acc)

    def turn(p, tile):
        tags = msg[p, 40:48, :]
        for v in range(CAP // 8):
            if v < 6:
                own = msg[p, 8 * v : 8 * v + 8, :]
            else:
                own = pltpu.roll(msg[p, 8 * v - 48 : 8 * v - 40, :], 64, 1)
            side = pltpu.roll(tags, 128 - 4 * v, 1) if v else tags
            tile[8 * v : 8 * v + 8, :] = jnp.where(low, own, side)

    turn(0, tiles[0])

    def step(k, carry):
        for i in range(32):
            if i % 8 == 0:
                index_copy(0, i // 8).wait()
            turn(jnp.minimum(32 * k + i + 1, PEERS - 1), tiles[(i + 1) % 4])
            tile = tiles[i % 4]
            for r in range(CAP):
                col = r // 8 * 4 + i % 8 % 4 + i % 8 // 4 * 64
                placed[pl.ds(slot_s[i // 8][r % 8, col], 1), :] = tile[r : r + 1, :]
            if i % 8 == 7:
                index_copy(jnp.minimum(4 * k + i // 8 + 4, PEERS // 8 - 1), i // 8).start()

        return carry

    lax.fori_loop(0, PEERS // 32, step, 0)
    for buf in range(4):
        index_copy(0, buf).wait()

    owned = iota((FOR_DEV, 128), 0)

    def out_copy(k):
        part = pl.ds(8 * k if isinstance(k, int) else pl.multiple_of(8 * k, 8), 8)
        return pltpu.make_async_copy(blocks.at[:, part, :], blocks_hbm.at[:, part, :], out_sems.at[k])

    def finish(k):
        highs, lows, members = [], [], []
        for h in range(8):
            b = 8 * k + h
            view = placed[b * 128 : b * 128 + 128, :].T
            x = view[:FIELDS]
            m = view[FIELDS : FIELDS + 1]
            by_row[pl.ds(b, FIELDS, stride=BLK_DEV), :] = x
            block_mass[b : b + 1, :] = m
            forest = view[FIELDS + 2 : FIELDS + 3].astype(jnp.int32)
            members.append((owned == forest).astype(jnp.float32).astype(jnp.bfloat16))
            scaled = m * x
            terms = jnp.concatenate([scaled, scaled * x, jnp.broadcast_to(m, (8, 128))], axis=0)
            high = terms.astype(jnp.bfloat16)
            highs.append(high)
            lows.append((terms - high.astype(jnp.float32)).astype(jnp.bfloat16))
        out_copy(k).start()
        member = jnp.concatenate(members, axis=1)
        for part in (highs, lows):
            acc[...] += lax.dot_general(
                jnp.concatenate(part, axis=1),
                member,
                (((1,), (1,)), ((), ())),
                preferred_element_type=jnp.float32,
            )

    for k in range(BLK_DEV // 8):
        finish(k)
    others = [
        pltpu.make_async_copy(src, dst, out_sems.at[BLK_DEV // 8 + n])
        for n, (src, dst) in enumerate(
            ((block_mass, block_mass_hbm), (fmass, fmass_hbm), (fmean, fmean_hbm), (fsecond, fsecond_hbm))
        )
    ]
    others[0].start()
    weight = acc[2 * FIELDS : 2 * FIELDS + 1]
    mass_total = jnp.broadcast_to(total[0:1, 127:128], (1, FOR_DEV))
    fmass[...] = weight * (FOR_DEV * PEERS / mass_total)
    others[1].start()
    fmean[...] = acc[:FIELDS] / weight
    others[2].start()
    fsecond[...] = acc[FIELDS : 2 * FIELDS] / weight
    others[3].start()
    for copy in [out_copy(k) for k in range(BLK_DEV // 8)] + others:
        copy.wait()


def pack(records, halo_mass, forest_id, dest_block, dest_slot):
    snaps, halos = halo_mass.shape
    groups = snaps * halos // 128

    def by_group(a):
        lead = a.shape[:-2]
        a = a.reshape(lead + (snaps, halos // 128, 128))
        return jnp.swapaxes(a, -3, -2).reshape(-1, 128)

    records, mass, forest, block, slot = map(by_group, (records, halo_mass, forest_id, dest_block, dest_slot))
    row = (groups, 128)
    vmem = pl.BlockSpec(memory_space=pltpu.VMEM)
    params = pltpu.CompilerParams(vmem_limit_bytes=VMEM_LIMIT)
    before, placed, slots = pl.pallas_call(
        init_kernel,
        out_shape=(
            jax.ShapeDtypeStruct((256, 384), jnp.bfloat16),
            jax.ShapeDtypeStruct((PEERS * CAP, 128), jnp.float32),
            jax.ShapeDtypeStruct((SLOTS + 128, 128), jnp.float32),
        ),
        out_specs=(vmem,) * 3,
        cost_estimate=pl.CostEstimate(flops=2**31, bytes_accessed=2**16, transcendentals=0),
        compiler_params=params,
        name="init",
    )()
    target, first_tag = pl.pallas_call(
        rank_kernel,
        out_shape=(jax.ShapeDtypeStruct(row, jnp.int32),) * 2,
        in_specs=[vmem] * 2,
        out_specs=(vmem,) * 2,
        cost_estimate=pl.CostEstimate(flops=2**20, bytes_accessed=2**16, transcendentals=0),
        compiler_params=params,
        name="rank",
    )(block, before)
    outbox, _ = pl.pallas_call(
        pack_kernel,
        out_shape=(
            jax.ShapeDtypeStruct((PEERS, ROWS, 128), jnp.float32),
            jax.ShapeDtypeStruct((PEERS * CAP, 128), jnp.float32),
        ),
        in_specs=[vmem] * 8,
        out_specs=(vmem, pl.BlockSpec(memory_space=pltpu.VMEM)),
        input_output_aliases={7: 1},
        scratch_shapes=[
            pltpu.VMEM(row, jnp.int32),
            pltpu.VMEM((FIELDS * PITCH, 128), jnp.float32),
            [pltpu.VMEM((128, 128), jnp.float32)] * 4,
            [pltpu.SMEM((8, 128), jnp.int32)] * (groups // 8),
            pltpu.SemaphoreType.DMA((groups // 8,)),
        ],
        compiler_params=params,
        name="pack",
    )(target, first_tag, records, mass, forest, block, slot, placed)
    return outbox, slots


def place(msg, slots):
    f32 = jnp.float32
    vmem = pl.BlockSpec(memory_space=pltpu.VMEM)
    shapes = ((FIELDS, BLK_DEV, 128), (BLK_DEV, 128), (1, FOR_DEV), (FIELDS, FOR_DEV), (FIELDS, FOR_DEV))
    return pl.pallas_call(
        place_kernel,
        out_shape=tuple(jax.ShapeDtypeStruct(shape, f32) for shape in shapes + (slots.shape,)),
        in_specs=[vmem] * 2,
        out_specs=(pl.BlockSpec(memory_space=pltpu.HBM),) * 5 + (vmem,),
        input_output_aliases={1: 5},
        scratch_shapes=[pltpu.VMEM(shape, f32) for shape in shapes]
        + [
            pltpu.VMEM((2 * FIELDS + 8, FOR_DEV), f32),
            [pltpu.VMEM((CAP, 128), f32)] * 4,
            pltpu.VMEM((PEERS, 128), jnp.int32),
            [pltpu.SMEM((8, 128), jnp.int32)] * 4,
            pltpu.SemaphoreType.DMA((4,)),
            pltpu.SemaphoreType.DMA((BLK_DEV // 8 + 4,)),
        ],
        compiler_params=pltpu.CompilerParams(vmem_limit_bytes=VMEM_LIMIT),
        name="place",
    )(msg, slots)[:5]


def on_device(records, halo_mass, forest_id, dest_block, dest_slot):
    outbox, slots = pack(records, halo_mass, forest_id, dest_block, dest_slot)
    inbox = lax.all_to_all(outbox, EXCHANGE, split_axis=0, concat_axis=0, tiled=True)
    blocks, block_mass, fmass, fmean, fsecond = place(inbox, slots)
    return blocks, block_mass, fmass.reshape(FOR_DEV), fmean, fsecond


def solution(mesh):
    split = Mesh(
        mesh.devices.reshape(mesh.shape["row"], mesh.shape["sa"], 2, 2, 2, 2),
        ROW_SA_HA,
    )
    in_specs = (
        P(None, "sa", ROW_HA),
        P("sa", ROW_HA),
        P("sa", ROW_HA),
        P("sa", ROW_HA),
        P("sa", ROW_HA),
    )
    out_specs = (
        P(None, ROW_SA_HA, None),
        P(ROW_SA_HA, None),
        P(ROW_SA_HA),
        P(None, ROW_SA_HA),
        P(None, ROW_SA_HA),
    )
    return jax.shard_map(
        on_device, mesh=split, in_specs=in_specs, out_specs=out_specs, check_vma=False
    )
```

```python
import jax
import jax.numpy as jnp
from jax import lax
from jax.experimental import pallas as pl
from jax.experimental.pallas import tpu as pltpu
from jax.sharding import Mesh
from jax.sharding import PartitionSpec as P

FIELDS = 64
FOR_DEV = 128
BLK_DEV = 40
SLOTS = BLK_DEV * 128
PEERS = 64
CAP = 88
ROWS = 48
TAGS = 48
PITCH = 40
VMEM_LIMIT = 24 * 1024 * 1024
EXCHANGE = ("core", "sa", "z0", "z1", "z2")
ROW_HA = ("row", "z2", "z1", "z0", "core")
ROW_SA_HA = ("row", "sa", "z2", "z1", "z0", "core")


def iota(shape, dim):
    return lax.broadcasted_iota(jnp.int32, shape, dim)


def owner_of(block):
    return lax.shift_right_logical(block * 1639, 16)


def position_of(owner):
    core = (owner & 1) << 5
    plane = lax.shift_right_logical(owner, 4) << 3
    turned = ((owner & 2) << 1) | lax.shift_right_logical(owner & 4, 1) | lax.shift_right_logical(owner & 8, 3)
    return core | plane | turned


def init_kernel(before, outbox, slots):
    ordered = (iota((256, 384), 0) < iota((256, 384), 1)) | (iota((256, 384), 1) >= 256)
    before[...] = ordered.astype(jnp.float32).astype(jnp.bfloat16)

    for array in (outbox, slots):

        def clear(k, carry):
            array[pl.ds(pl.multiple_of(k * 128, 128), 128), :] = jnp.zeros((128, 128), jnp.float32)
            return carry

        lax.fori_loop(0, array.shape[0] // 128, clear, 0)


def rank_kernel(block, before, target, first_tag):
    groups = block.shape[0]
    peer = iota((PEERS, 128), 0)
    base = jnp.zeros((PEERS, 128), jnp.float32)
    goal = position_of(owner_of(block[...]))
    for g in range(0, groups, 2):
        member = jnp.concatenate([peer == goal[g : g + 1], peer == goal[g + 1 : g + 2]], axis=1)
        counts = jnp.dot(
            member.astype(jnp.float32).astype(jnp.bfloat16), before[...], preferred_element_type=jnp.float32
        )
        rank = counts[:, :256] + jnp.concatenate([base, base], axis=1)
        rank = jnp.sum(jnp.where(member, rank, 0.0), axis=0, keepdims=True).astype(jnp.int32)
        base = base + counts[:, 256:]
        first_tag[g : g + 1, :] = rank[:, :128]
        first_tag[g + 1 : g + 2, :] = rank[:, 128:]
    rank = first_tag[...]
    target[...] = goal * CAP + rank
    first_tag[...] = lax.shift_right_logical(rank, 3) << 2


def pack_kernel(
    target_v, first_tag, rec, mass, forest, block, slot_in, start, out, placed, slot, spaced, tiles, target_s, sems
):
    del start
    groups = mass.shape[0]

    def index_copy(k):
        return pltpu.make_async_copy(target_v.at[8 * k : 8 * k + 8, :], target_s[k], sems.at[k])

    for k in range(groups // 8):
        index_copy(k).start()
    for tile in tiles:
        tile[...] = jnp.zeros_like(tile)
    slot[...] = (block[...] - owner_of(block[...]) * BLK_DEV) * 128 + slot_in[...] + 1

    for f in range(FIELDS):
        spaced[PITCH * f : PITCH * f + groups, :] = rec[groups * f : groups * f + groups, :]
    line = iota((TAGS, 128), 0)

    def turn(group, tile):
        def row(ref):
            return jnp.broadcast_to(ref[pl.ds(group, 1), :], (TAGS, 128))

        own_line = line - row(first_tag)
        tags = jnp.where(own_line == 0, row(mass), 0.0)
        tags = jnp.where(own_line == 1, row(slot).astype(jnp.float32), tags)
        tags = jnp.where(own_line == 2, (row(forest) & (FOR_DEV - 1)).astype(jnp.float32), tags)
        stack = jnp.concatenate([spaced[pl.ds(group, FIELDS, stride=PITCH), :], tags], axis=0)
        tile[:, : FIELDS + TAGS] = stack.T

    turn(0, tiles[0])

    for i in range(groups):
        if i % 8 == 0:
            index_copy(i // 8).wait()
        if i + 1 < groups:
            turn(i + 1, tiles[(i + 1) % 4])
        tile = tiles[i % 4]
        for r in range(128):
            placed[pl.ds(target_s[i // 8][i % 8, r], 1), :] = tile[r : r + 1, :]

    lane = iota((8, 128), 1)
    low = lane < FIELDS
    total = jnp.sum(jnp.sum(mass[...], axis=0, keepdims=True), axis=1, keepdims=True)
    corner = jnp.where(lane == 127, jnp.broadcast_to(total, (8, 128)), 0.0)

    def squeeze(k, carry):
        for h in range(16):
            p = 16 * k + h
            start = p * CAP
            rows = [placed[pl.ds(pl.multiple_of(start + 8 * v, 8), 8), :] for v in range(CAP // 8)]
            for v in range(5):
                out[p, 8 * v : 8 * v + 8, :] = jnp.where(low, rows[v], pltpu.roll(rows[v + 6], 64, 1))
            tags = corner
            for row in rows:
                tags = tags + row
            out[p, 40:48, :] = jnp.where(low, rows[5], tags)
        return carry

    lax.fori_loop(0, PEERS // 16, squeeze, 0)


def place_kernel(
    msg, start, blocks_hbm, block_mass_hbm, fmass_hbm, fmean_hbm, fsecond_hbm, placed,
    blocks, block_mass, fmass, fmean, fsecond, acc, tiles, slot_v, slot_s, sems, out_sems,
):
    del start
    by_row = blocks.reshape(FIELDS * BLK_DEV, 128)

    def index_copy(g, buf):
        return pltpu.make_async_copy(
            slot_v.at[pl.ds(pl.multiple_of(8 * g, 8), 8), :], slot_s[buf], sems.at[buf]
        )

    lane = iota((8, 128), 1)
    low = lane < FIELDS
    slot_lane = (lane >= FIELDS) & (lane < FIELDS + 4 * (CAP // 8)) & (lane % 4 == 1)
    total = jnp.zeros((8, 128), jnp.float32)
    for g in range(PEERS // 8):
        index = jnp.zeros((8, 128), jnp.float32)
        for k in range(8):
            tags = msg[8 * g + k, 40:48, :]
            total = total + tags
            index = index + pltpu.roll(
                jnp.where(slot_lane, tags, 0.0), (64 * (k // 4) + k % 4 - 65) % 128, 1
            )
        index = index.astype(jnp.int32)
        slot_v[8 * g : 8 * g + 8, :] = jnp.where(index == 0, SLOTS, index - 1)
        if g < 4:
            index_copy(g, g).start()
    acc[...] = jnp.zeros_like(acc)

    def turn(p, tile):
        tags = msg[p, 40:48, :]
        for v in range(CAP // 8):
            if v < 6:
                own = msg[p, 8 * v : 8 * v + 8, :]
            else:
                own = pltpu.roll(msg[p, 8 * v - 48 : 8 * v - 40, :], 64, 1)
            side = pltpu.roll(tags, 128 - 4 * v, 1) if v else tags
            tile[8 * v : 8 * v + 8, :] = jnp.where(low, own, side)

    turn(0, tiles[0])
    turn(1, tiles[1])

    def step(k, carry):
        for i in range(32):
            if i % 8 == 0:
                index_copy(0, i // 8).wait()
            turn(jnp.minimum(32 * k + i + 2, PEERS - 1), tiles[(i + 2) % 4])
            tile = tiles[i % 4]
            for r in range(CAP):
                col = r // 8 * 4 + i % 8 % 4 + i % 8 // 4 * 64
                placed[pl.ds(slot_s[i // 8][r % 8, col], 1), :] = tile[r : r + 1, :]
            if i % 8 == 7:
                index_copy(jnp.minimum(4 * k + i // 8 + 4, PEERS // 8 - 1), i // 8).start()

        return carry

    lax.fori_loop(0, PEERS // 32, step, 0)
    for buf in range(4):
        index_copy(0, buf).wait()

    owned = iota((FOR_DEV, 128), 0)

    def out_copy(k):
        part = pl.ds(8 * k if isinstance(k, int) else pl.multiple_of(8 * k, 8), 8)
        return pltpu.make_async_copy(blocks.at[:, part, :], blocks_hbm.at[:, part, :], out_sems.at[k])

    def finish(k):
        highs, lows, members = [], [], []
        for h in range(8):
            b = 8 * k + h
            view = placed[b * 128 : b * 128 + 128, :].T
            x = view[:FIELDS]
            m = view[FIELDS : FIELDS + 1]
            by_row[pl.ds(b, FIELDS, stride=BLK_DEV), :] = x
            block_mass[b : b + 1, :] = m
            forest = view[FIELDS + 2 : FIELDS + 3].astype(jnp.int32)
            members.append((owned == forest).astype(jnp.float32).astype(jnp.bfloat16))
            scaled = m * x
            terms = jnp.concatenate([scaled, scaled * x, jnp.broadcast_to(m, (8, 128))], axis=0)
            high = terms.astype(jnp.bfloat16)
            highs.append(high)
            lows.append((terms - high.astype(jnp.float32)).astype(jnp.bfloat16))
        out_copy(k).start()
        member = jnp.concatenate(members, axis=1)
        for part in (highs, lows):
            acc[...] += lax.dot_general(
                jnp.concatenate(part, axis=1),
                member,
                (((1,), (1,)), ((), ())),
                preferred_element_type=jnp.float32,
            )

    for k in range(BLK_DEV // 8):
        finish(k)
    others = [
        pltpu.make_async_copy(src, dst, out_sems.at[BLK_DEV // 8 + n])
        for n, (src, dst) in enumerate(
            ((block_mass, block_mass_hbm), (fmass, fmass_hbm), (fmean, fmean_hbm), (fsecond, fsecond_hbm))
        )
    ]
    others[0].start()
    weight = acc[2 * FIELDS : 2 * FIELDS + 1]
    mass_total = jnp.broadcast_to(total[0:1, 127:128], (1, FOR_DEV))
    fmass[...] = weight * (FOR_DEV * PEERS / mass_total)
    others[1].start()
    fmean[...] = acc[:FIELDS] / weight
    others[2].start()
    fsecond[...] = acc[FIELDS : 2 * FIELDS] / weight
    others[3].start()
    for copy in [out_copy(k) for k in range(BLK_DEV // 8)] + others:
        copy.wait()


def pack(records, halo_mass, forest_id, dest_block, dest_slot):
    snaps, halos = halo_mass.shape
    groups = snaps * halos // 128

    def by_group(a):
        lead = a.shape[:-2]
        a = a.reshape(lead + (snaps, halos // 128, 128))
        return jnp.swapaxes(a, -3, -2).reshape(-1, 128)

    records, mass, forest, block, slot = map(by_group, (records, halo_mass, forest_id, dest_block, dest_slot))
    row = (groups, 128)
    vmem = pl.BlockSpec(memory_space=pltpu.VMEM)
    params = pltpu.CompilerParams(vmem_limit_bytes=VMEM_LIMIT)
    before, placed, slots = pl.pallas_call(
        init_kernel,
        out_shape=(
            jax.ShapeDtypeStruct((256, 384), jnp.bfloat16),
            jax.ShapeDtypeStruct((PEERS * CAP, 128), jnp.float32),
            jax.ShapeDtypeStruct((SLOTS + 128, 128), jnp.float32),
        ),
        out_specs=(vmem,) * 3,
        cost_estimate=pl.CostEstimate(flops=2**31, bytes_accessed=2**16, transcendentals=0),
        compiler_params=params,
        name="init",
    )()
    target, first_tag = pl.pallas_call(
        rank_kernel,
        out_shape=(jax.ShapeDtypeStruct(row, jnp.int32),) * 2,
        in_specs=[vmem] * 2,
        out_specs=(vmem,) * 2,
        cost_estimate=pl.CostEstimate(flops=2**20, bytes_accessed=2**16, transcendentals=0),
        compiler_params=params,
        name="rank",
    )(block, before)
    outbox, _ = pl.pallas_call(
        pack_kernel,
        out_shape=(
            jax.ShapeDtypeStruct((PEERS, ROWS, 128), jnp.float32),
            jax.ShapeDtypeStruct((PEERS * CAP, 128), jnp.float32),
        ),
        in_specs=[vmem] * 8,
        out_specs=(vmem, pl.BlockSpec(memory_space=pltpu.VMEM)),
        input_output_aliases={7: 1},
        scratch_shapes=[
            pltpu.VMEM(row, jnp.int32),
            pltpu.VMEM((FIELDS * PITCH, 128), jnp.float32),
            [pltpu.VMEM((128, 128), jnp.float32)] * 4,
            [pltpu.SMEM((8, 128), jnp.int32)] * (groups // 8),
            pltpu.SemaphoreType.DMA((groups // 8,)),
        ],
        compiler_params=params,
        name="pack",
    )(target, first_tag, records, mass, forest, block, slot, placed)
    return outbox, slots


def place(msg, slots):
    f32 = jnp.float32
    vmem = pl.BlockSpec(memory_space=pltpu.VMEM)
    shapes = ((FIELDS, BLK_DEV, 128), (BLK_DEV, 128), (1, FOR_DEV), (FIELDS, FOR_DEV), (FIELDS, FOR_DEV))
    return pl.pallas_call(
        place_kernel,
        out_shape=tuple(jax.ShapeDtypeStruct(shape, f32) for shape in shapes + (slots.shape,)),
        in_specs=[vmem] * 2,
        out_specs=(pl.BlockSpec(memory_space=pltpu.HBM),) * 5 + (vmem,),
        input_output_aliases={1: 5},
        scratch_shapes=[pltpu.VMEM(shape, f32) for shape in shapes]
        + [
            pltpu.VMEM((2 * FIELDS + 8, FOR_DEV), f32),
            [pltpu.VMEM((CAP, 128), f32)] * 4,
            pltpu.VMEM((PEERS, 128), jnp.int32),
            [pltpu.SMEM((8, 128), jnp.int32)] * 4,
            pltpu.SemaphoreType.DMA((4,)),
            pltpu.SemaphoreType.DMA((BLK_DEV // 8 + 4,)),
        ],
        compiler_params=pltpu.CompilerParams(vmem_limit_bytes=VMEM_LIMIT),
        name="place",
    )(msg, slots)[:5]


def on_device(records, halo_mass, forest_id, dest_block, dest_slot):
    outbox, slots = pack(records, halo_mass, forest_id, dest_block, dest_slot)
    inbox = lax.all_to_all(outbox, EXCHANGE, split_axis=0, concat_axis=0, tiled=True)
    blocks, block_mass, fmass, fmean, fsecond = place(inbox, slots)
    return blocks, block_mass, fmass.reshape(FOR_DEV), fmean, fsecond


def solution(mesh):
    split = Mesh(
        mesh.devices.reshape(mesh.shape["row"], mesh.shape["sa"], 2, 2, 2, 2),
        ROW_SA_HA,
    )
    in_specs = (
        P(None, "sa", ROW_HA),
        P("sa", ROW_HA),
        P("sa", ROW_HA),
        P("sa", ROW_HA),
        P("sa", ROW_HA),
    )
    out_specs = (
        P(None, ROW_SA_HA, None),
        P(ROW_SA_HA, None),
        P(ROW_SA_HA),
        P(None, ROW_SA_HA),
        P(None, ROW_SA_HA),
    )
    return jax.shard_map(
        on_device, mesh=split, in_specs=in_specs, out_specs=out_specs, check_vma=False
    )
```

```python
import jax
import jax.numpy as jnp
from jax import lax
from jax.experimental import pallas as pl
from jax.experimental.pallas import tpu as pltpu
from jax.sharding import Mesh
from jax.sharding import PartitionSpec as P

FIELDS = 64
FOR_DEV = 128
BLK_DEV = 40
SLOTS = BLK_DEV * 128
PEERS = 64
CAP = 88
ROWS = 48
TAGS = 48
PITCH = 40
VMEM_LIMIT = 24 * 1024 * 1024
EXCHANGE = ("core", "sa", "z0", "z1", "z2")
ROW_HA = ("row", "z2", "z1", "z0", "core")
ROW_SA_HA = ("row", "sa", "z2", "z1", "z0", "core")


def iota(shape, dim):
    return lax.broadcasted_iota(jnp.int32, shape, dim)


def owner_of(block):
    return lax.shift_right_logical(block * 1639, 16)


def position_of(owner):
    core = (owner & 1) << 5
    plane = lax.shift_right_logical(owner, 4) << 3
    turned = ((owner & 2) << 1) | lax.shift_right_logical(owner & 4, 1) | lax.shift_right_logical(owner & 8, 3)
    return core | plane | turned


def init_kernel(before, outbox, slots):
    ordered = (iota((256, 384), 0) < iota((256, 384), 1)) | (iota((256, 384), 1) >= 256)
    before[...] = ordered.astype(jnp.float32).astype(jnp.bfloat16)

    for array in (outbox, slots):

        def clear(k, carry):
            array[pl.ds(pl.multiple_of(k * 128, 128), 128), :] = jnp.zeros((128, 128), jnp.float32)
            return carry

        lax.fori_loop(0, array.shape[0] // 128, clear, 0)


def rank_kernel(block, before, target, first_tag):
    groups = block.shape[0]
    peer = iota((PEERS, 128), 0)
    base = jnp.zeros((PEERS, 128), jnp.float32)
    goal = position_of(owner_of(block[...]))
    for g in range(0, groups, 2):
        member = jnp.concatenate([peer == goal[g : g + 1], peer == goal[g + 1 : g + 2]], axis=1)
        counts = jnp.dot(
            member.astype(jnp.float32).astype(jnp.bfloat16), before[...], preferred_element_type=jnp.float32
        )
        rank = counts[:, :256] + jnp.concatenate([base, base], axis=1)
        rank = jnp.sum(jnp.where(member, rank, 0.0), axis=0, keepdims=True).astype(jnp.int32)
        base = base + counts[:, 256:]
        first_tag[g : g + 1, :] = rank[:, :128]
        first_tag[g + 1 : g + 2, :] = rank[:, 128:]
    rank = first_tag[...]
    target[...] = goal * CAP + rank
    first_tag[...] = lax.shift_right_logical(rank, 3) << 2


def pack_kernel(
    target_v, first_tag, rec, mass, forest, block, slot_in, start, out, placed, slot, spaced, tiles, target_s, sems
):
    del start
    groups = mass.shape[0]

    def index_copy(k):
        return pltpu.make_async_copy(target_v.at[8 * k : 8 * k + 8, :], target_s[k], sems.at[k])

    for k in range(groups // 8):
        index_copy(k).start()
    for tile in tiles:
        tile[...] = jnp.zeros_like(tile)
    slot[...] = (block[...] - owner_of(block[...]) * BLK_DEV) * 128 + slot_in[...] + 1

    for f in range(FIELDS):
        spaced[PITCH * f : PITCH * f + groups, :] = rec[groups * f : groups * f + groups, :]
    line = iota((TAGS, 128), 0)

    def turn(group, tile):
        def row(ref):
            return jnp.broadcast_to(ref[pl.ds(group, 1), :], (TAGS, 128))

        own_line = line - row(first_tag)
        tags = jnp.where(own_line == 0, row(mass), 0.0)
        tags = jnp.where(own_line == 1, row(slot).astype(jnp.float32), tags)
        tags = jnp.where(own_line == 2, (row(forest) & (FOR_DEV - 1)).astype(jnp.float32), tags)
        stack = jnp.concatenate([spaced[pl.ds(group, FIELDS, stride=PITCH), :], tags], axis=0)
        tile[:, : FIELDS + TAGS] = stack.T

    turn(0, tiles[0])

    for i in range(groups):
        if i == 0:
            for k in range(groups // 8):
                index_copy(k).wait()
        if i + 1 < groups:
            turn(i + 1, tiles[(i + 1) % 4])
        tile = tiles[i % 4]
        for r in range(128):
            placed[pl.ds(target_s[i // 8][i % 8, r], 1), :] = tile[r : r + 1, :]

    lane = iota((8, 128), 1)
    low = lane < FIELDS
    total = jnp.sum(jnp.sum(mass[...], axis=0, keepdims=True), axis=1, keepdims=True)
    corner = jnp.where(lane == 127, jnp.broadcast_to(total, (8, 128)), 0.0)

    def squeeze(k, carry):
        for h in range(16):
            p = 16 * k + h
            start = p * CAP
            rows = [placed[pl.ds(pl.multiple_of(start + 8 * v, 8), 8), :] for v in range(CAP // 8)]
            for v in range(5):
                out[p, 8 * v : 8 * v + 8, :] = jnp.where(low, rows[v], pltpu.roll(rows[v + 6], 64, 1))
            tags = corner
            for row in rows:
                tags = tags + row
            out[p, 40:48, :] = jnp.where(low, rows[5], tags)
        return carry

    lax.fori_loop(0, PEERS // 16, squeeze, 0)


def place_kernel(
    msg, start, blocks_hbm, block_mass_hbm, fmass_hbm, fmean_hbm, fsecond_hbm, placed,
    blocks, block_mass, fmass, fmean, fsecond, acc, tiles, slot_v, slot_s, sems, out_sems,
):
    del start
    by_row = blocks.reshape(FIELDS * BLK_DEV, 128)

    def index_copy(g):
        return pltpu.make_async_copy(slot_v.at[8 * g : 8 * g + 8, :], slot_s[g], sems.at[g])

    lane = iota((8, 128), 1)
    low = lane < FIELDS
    slot_lane = (lane >= FIELDS) & (lane < FIELDS + 4 * (CAP // 8)) & (lane % 4 == 1)
    total = jnp.zeros((8, 128), jnp.float32)
    for g in range(PEERS // 8):
        index = jnp.zeros((8, 128), jnp.float32)
        for k in range(8):
            tags = msg[8 * g + k, 40:48, :]
            total = total + tags
            index = index + pltpu.roll(
                jnp.where(slot_lane, tags, 0.0), (64 * (k // 4) + k % 4 - 65) % 128, 1
            )
        index = index.astype(jnp.int32)
        slot_v[8 * g : 8 * g + 8, :] = jnp.where(index == 0, SLOTS, index - 1)
        index_copy(g).start()
    acc[...] = jnp.zeros_like(acc)

    def turn(p, tile):
        tags = msg[p, 40:48, :]
        for v in range(CAP // 8):
            if v < 6:
                own = msg[p, 8 * v : 8 * v + 8, :]
            else:
                own = pltpu.roll(msg[p, 8 * v - 48 : 8 * v - 40, :], 64, 1)
            side = pltpu.roll(tags, 128 - 4 * v, 1) if v else tags
            tile[8 * v : 8 * v + 8, :] = jnp.where(low, own, side)

    turn(0, tiles[0])
    turn(1, tiles[1])

    for g in range(PEERS // 8):
        index_copy(g).wait()
    for i in range(PEERS):
        if i + 2 < PEERS:
            turn(i + 2, tiles[(i + 2) % 4])
        tile = tiles[i % 4]
        for r in range(CAP):
            col = r // 8 * 4 + i % 8 % 4 + i % 8 // 4 * 64
            placed[pl.ds(slot_s[i // 8][r % 8, col], 1), :] = tile[r : r + 1, :]

    owned = iota((FOR_DEV, 128), 0)

    def out_copy(k):
        part = pl.ds(8 * k if isinstance(k, int) else pl.multiple_of(8 * k, 8), 8)
        return pltpu.make_async_copy(blocks.at[:, part, :], blocks_hbm.at[:, part, :], out_sems.at[k])

    def finish(k):
        highs, lows, members = [], [], []
        for h in range(8):
            b = 8 * k + h
            view = placed[b * 128 : b * 128 + 128, :].T
            x = view[:FIELDS]
            m = view[FIELDS : FIELDS + 1]
            by_row[pl.ds(b, FIELDS, stride=BLK_DEV), :] = x
            block_mass[b : b + 1, :] = m
            forest = view[FIELDS + 2 : FIELDS + 3].astype(jnp.int32)
            members.append((owned == forest).astype(jnp.float32).astype(jnp.bfloat16))
            scaled = m * x
            terms = jnp.concatenate([scaled, scaled * x, jnp.broadcast_to(m, (8, 128))], axis=0)
            high = terms.astype(jnp.bfloat16)
            highs.append(high)
            lows.append((terms - high.astype(jnp.float32)).astype(jnp.bfloat16))
        out_copy(k).start()
        member = jnp.concatenate(members, axis=1)
        for part in (highs, lows):
            acc[...] += lax.dot_general(
                jnp.concatenate(part, axis=1),
                member,
                (((1,), (1,)), ((), ())),
                preferred_element_type=jnp.float32,
            )

    for k in range(BLK_DEV // 8):
        finish(k)
    others = [
        pltpu.make_async_copy(src, dst, out_sems.at[BLK_DEV // 8 + n])
        for n, (src, dst) in enumerate(
            ((block_mass, block_mass_hbm), (fmass, fmass_hbm), (fmean, fmean_hbm), (fsecond, fsecond_hbm))
        )
    ]
    others[0].start()
    weight = acc[2 * FIELDS : 2 * FIELDS + 1]
    mass_total = jnp.broadcast_to(total[0:1, 127:128], (1, FOR_DEV))
    fmass[...] = weight * (FOR_DEV * PEERS / mass_total)
    others[1].start()
    fmean[...] = acc[:FIELDS] / weight
    others[2].start()
    fsecond[...] = acc[FIELDS : 2 * FIELDS] / weight
    others[3].start()
    for copy in [out_copy(k) for k in range(BLK_DEV // 8)] + others:
        copy.wait()


def pack(records, halo_mass, forest_id, dest_block, dest_slot):
    snaps, halos = halo_mass.shape
    groups = snaps * halos // 128

    def by_group(a):
        lead = a.shape[:-2]
        a = a.reshape(lead + (snaps, halos // 128, 128))
        return jnp.swapaxes(a, -3, -2).reshape(-1, 128)

    records, mass, forest, block, slot = map(by_group, (records, halo_mass, forest_id, dest_block, dest_slot))
    row = (groups, 128)
    vmem = pl.BlockSpec(memory_space=pltpu.VMEM)
    params = pltpu.CompilerParams(vmem_limit_bytes=VMEM_LIMIT)
    before, placed, slots = pl.pallas_call(
        init_kernel,
        out_shape=(
            jax.ShapeDtypeStruct((256, 384), jnp.bfloat16),
            jax.ShapeDtypeStruct((PEERS * CAP, 128), jnp.float32),
            jax.ShapeDtypeStruct((SLOTS + 128, 128), jnp.float32),
        ),
        out_specs=(vmem,) * 3,
        cost_estimate=pl.CostEstimate(flops=2**31, bytes_accessed=2**16, transcendentals=0),
        compiler_params=params,
        name="init",
    )()
    target, first_tag = pl.pallas_call(
        rank_kernel,
        out_shape=(jax.ShapeDtypeStruct(row, jnp.int32),) * 2,
        in_specs=[vmem] * 2,
        out_specs=(vmem,) * 2,
        cost_estimate=pl.CostEstimate(flops=2**20, bytes_accessed=2**16, transcendentals=0),
        compiler_params=params,
        name="rank",
    )(block, before)
    outbox, _ = pl.pallas_call(
        pack_kernel,
        out_shape=(
            jax.ShapeDtypeStruct((PEERS, ROWS, 128), jnp.float32),
            jax.ShapeDtypeStruct((PEERS * CAP, 128), jnp.float32),
        ),
        in_specs=[vmem] * 8,
        out_specs=(vmem, pl.BlockSpec(memory_space=pltpu.VMEM)),
        input_output_aliases={7: 1},
        scratch_shapes=[
            pltpu.VMEM(row, jnp.int32),
            pltpu.VMEM((FIELDS * PITCH, 128), jnp.float32),
            [pltpu.VMEM((128, 128), jnp.float32)] * 4,
            [pltpu.SMEM((8, 128), jnp.int32)] * (groups // 8),
            pltpu.SemaphoreType.DMA((groups // 8,)),
        ],
        compiler_params=params,
        name="pack",
    )(target, first_tag, records, mass, forest, block, slot, placed)
    return outbox, slots


def place(msg, slots):
    f32 = jnp.float32
    vmem = pl.BlockSpec(memory_space=pltpu.VMEM)
    shapes = ((FIELDS, BLK_DEV, 128), (BLK_DEV, 128), (1, FOR_DEV), (FIELDS, FOR_DEV), (FIELDS, FOR_DEV))
    return pl.pallas_call(
        place_kernel,
        out_shape=tuple(jax.ShapeDtypeStruct(shape, f32) for shape in shapes + (slots.shape,)),
        in_specs=[vmem] * 2,
        out_specs=(pl.BlockSpec(memory_space=pltpu.HBM),) * 5 + (vmem,),
        input_output_aliases={1: 5},
        scratch_shapes=[pltpu.VMEM(shape, f32) for shape in shapes]
        + [
            pltpu.VMEM((2 * FIELDS + 8, FOR_DEV), f32),
            [pltpu.VMEM((CAP, 128), f32)] * 4,
            pltpu.VMEM((PEERS, 128), jnp.int32),
            [pltpu.SMEM((8, 128), jnp.int32)] * (PEERS // 8),
            pltpu.SemaphoreType.DMA((PEERS // 8,)),
            pltpu.SemaphoreType.DMA((BLK_DEV // 8 + 4,)),
        ],
        compiler_params=pltpu.CompilerParams(vmem_limit_bytes=VMEM_LIMIT),
        name="place",
    )(msg, slots)[:5]


def on_device(records, halo_mass, forest_id, dest_block, dest_slot):
    outbox, slots = pack(records, halo_mass, forest_id, dest_block, dest_slot)
    inbox = lax.all_to_all(outbox, EXCHANGE, split_axis=0, concat_axis=0, tiled=True)
    blocks, block_mass, fmass, fmean, fsecond = place(inbox, slots)
    return blocks, block_mass, fmass.reshape(FOR_DEV), fmean, fsecond


def solution(mesh):
    split = Mesh(
        mesh.devices.reshape(mesh.shape["row"], mesh.shape["sa"], 2, 2, 2, 2),
        ROW_SA_HA,
    )
    in_specs = (
        P(None, "sa", ROW_HA),
        P("sa", ROW_HA),
        P("sa", ROW_HA),
        P("sa", ROW_HA),
        P("sa", ROW_HA),
    )
    out_specs = (
        P(None, ROW_SA_HA, None),
        P(ROW_SA_HA, None),
        P(ROW_SA_HA),
        P(None, ROW_SA_HA),
        P(None, ROW_SA_HA),
    )
    return jax.shard_map(
        on_device, mesh=split, in_specs=in_specs, out_specs=out_specs, check_vma=False
    )
```

```python
import jax
import jax.numpy as jnp
from jax import lax
from jax.experimental import pallas as pl
from jax.experimental.pallas import tpu as pltpu
from jax.sharding import Mesh
from jax.sharding import PartitionSpec as P

FIELDS = 64
FOR_DEV = 128
BLK_DEV = 40
SLOTS = BLK_DEV * 128
PEERS = 64
CAP = 88
ROWS = 48
TAGS = 48
PITCH = 40
VMEM_LIMIT = 24 * 1024 * 1024
EXCHANGE = ("core", "sa", "z0", "z1", "z2")
ROW_HA = ("row", "z2", "z1", "z0", "core")
ROW_SA_HA = ("row", "sa", "z2", "z1", "z0", "core")


def iota(shape, dim):
    return lax.broadcasted_iota(jnp.int32, shape, dim)


def owner_of(block):
    return lax.shift_right_logical(block * 1639, 16)


def position_of(owner):
    core = (owner & 1) << 5
    plane = lax.shift_right_logical(owner, 4) << 3
    turned = ((owner & 2) << 1) | lax.shift_right_logical(owner & 4, 1) | lax.shift_right_logical(owner & 8, 3)
    return core | plane | turned


def init_kernel(before, outbox, slots):
    ordered = (iota((256, 384), 0) < iota((256, 384), 1)) | (iota((256, 384), 1) >= 256)
    before[...] = ordered.astype(jnp.float32).astype(jnp.bfloat16)

    for array in (outbox, slots):

        def clear(k, carry):
            array[pl.ds(pl.multiple_of(k * 128, 128), 128), :] = jnp.zeros((128, 128), jnp.float32)
            return carry

        lax.fori_loop(0, array.shape[0] // 128, clear, 0)


def rank_kernel(block, before, target, first_tag):
    groups = block.shape[0]
    peer = iota((PEERS, 128), 0)
    base = jnp.zeros((PEERS, 128), jnp.float32)
    goal = position_of(owner_of(block[...]))
    for g in range(0, groups, 2):
        member = jnp.concatenate([peer == goal[g : g + 1], peer == goal[g + 1 : g + 2]], axis=1)
        counts = jnp.dot(
            member.astype(jnp.float32).astype(jnp.bfloat16), before[...], preferred_element_type=jnp.float32
        )
        rank = counts[:, :256] + jnp.concatenate([base, base], axis=1)
        rank = jnp.sum(jnp.where(member, rank, 0.0), axis=0, keepdims=True).astype(jnp.int32)
        base = base + counts[:, 256:]
        first_tag[g : g + 1, :] = rank[:, :128]
        first_tag[g + 1 : g + 2, :] = rank[:, 128:]
    rank = first_tag[...]
    target[...] = goal * CAP + rank
    first_tag[...] = lax.shift_right_logical(rank, 3) << 2


def pack_kernel(
    target_v, first_tag, rec, mass, forest, block, slot_in, start, out, placed, slot, spaced, tiles, target_s, sems
):
    del start
    groups = mass.shape[0]

    def index_copy(k):
        return pltpu.make_async_copy(target_v.at[8 * k : 8 * k + 8, :], target_s[k], sems.at[k])

    for k in range(groups // 8):
        index_copy(k).start()
    for tile in tiles:
        tile[...] = jnp.zeros_like(tile)
    slot[...] = (block[...] - owner_of(block[...]) * BLK_DEV) * 128 + slot_in[...] + 1

    for f in range(FIELDS):
        spaced[PITCH * f : PITCH * f + groups, :] = rec[groups * f : groups * f + groups, :]
    line = iota((TAGS, 128), 0)

    def turn(group, tile):
        def row(ref):
            return jnp.broadcast_to(ref[pl.ds(group, 1), :], (TAGS, 128))

        own_line = line - row(first_tag)
        tags = jnp.where(own_line == 0, row(mass), 0.0)
        tags = jnp.where(own_line == 1, row(slot).astype(jnp.float32), tags)
        tags = jnp.where(own_line == 2, (row(forest) & (FOR_DEV - 1)).astype(jnp.float32), tags)
        stack = jnp.concatenate([spaced[pl.ds(group, FIELDS, stride=PITCH), :], tags], axis=0)
        tile[:, : FIELDS + TAGS] = stack.T

    turn(0, tiles[0])

    for i in range(groups):
        if i % 8 == 0:
            index_copy(i // 8).wait()
        if i + 1 < groups:
            turn(i + 1, tiles[(i + 1) % 4])
        tile = tiles[i % 4]
        for r in range(128):
            placed[pl.ds(target_s[i // 8][i % 8, r], 1), :] = tile[r : r + 1, :]

    lane = iota((8, 128), 1)
    low = lane < FIELDS
    total = jnp.sum(jnp.sum(mass[...], axis=0, keepdims=True), axis=1, keepdims=True)
    corner = jnp.where(lane == 127, jnp.broadcast_to(total, (8, 128)), 0.0)

    def squeeze(k, carry):
        for h in range(16):
            p = 16 * k + h
            start = p * CAP
            rows = [placed[pl.ds(pl.multiple_of(start + 8 * v, 8), 8), :] for v in range(CAP // 8)]
            for v in range(5):
                out[p, 8 * v : 8 * v + 8, :] = jnp.where(low, rows[v], pltpu.roll(rows[v + 6], 64, 1))
            tags = corner
            for row in rows:
                tags = tags + row
            out[p, 40:48, :] = jnp.where(low, rows[5], tags)
        return carry

    lax.fori_loop(0, PEERS // 16, squeeze, 0)


def place_kernel(
    msg, start, blocks_hbm, block_mass_hbm, fmass_hbm, fmean_hbm, fsecond_hbm, placed,
    blocks, block_mass, fmass, fmean, fsecond, acc, tiles, slot_v, slot_s, sems, out_sems,
):
    del start
    by_row = blocks.reshape(FIELDS * BLK_DEV, 128)

    def index_copy(g):
        return pltpu.make_async_copy(slot_v.at[8 * g : 8 * g + 8, :], slot_s[g], sems.at[g])

    lane = iota((8, 128), 1)
    low = lane < FIELDS
    slot_lane = (lane >= FIELDS) & (lane < FIELDS + 4 * (CAP // 8)) & (lane % 4 == 1)
    total = jnp.zeros((8, 128), jnp.float32)
    for g in range(PEERS // 8):
        index = jnp.zeros((8, 128), jnp.float32)
        for k in range(8):
            tags = msg[8 * g + k, 40:48, :]
            total = total + tags
            index = index + pltpu.roll(
                jnp.where(slot_lane, tags, 0.0), (64 * (k // 4) + k % 4 - 65) % 128, 1
            )
        index = index.astype(jnp.int32)
        slot_v[8 * g : 8 * g + 8, :] = jnp.where(index == 0, SLOTS, index - 1)
        index_copy(g).start()
    acc[...] = jnp.zeros_like(acc)

    def turn(p, tile):
        tags = msg[p, 40:48, :]
        for v in range(CAP // 8):
            if v < 6:
                own = msg[p, 8 * v : 8 * v + 8, :]
            else:
                own = pltpu.roll(msg[p, 8 * v - 48 : 8 * v - 40, :], 64, 1)
            side = pltpu.roll(tags, 128 - 4 * v, 1) if v else tags
            tile[8 * v : 8 * v + 8, :] = jnp.where(low, own, side)

    turn(0, tiles[0])
    turn(1, tiles[1])

    for i in range(PEERS):
        if i == 0:
            index_copy(0).wait()
        if i == 8:
            for g in range(1, PEERS // 8):
                index_copy(g).wait()
        if i + 2 < PEERS:
            turn(i + 2, tiles[(i + 2) % 4])
        tile = tiles[i % 4]
        for r in range(CAP):
            col = r // 8 * 4 + i % 8 % 4 + i % 8 // 4 * 64
            placed[pl.ds(slot_s[i // 8][r % 8, col], 1), :] = tile[r : r + 1, :]

    owned = iota((FOR_DEV, 128), 0)

    def out_copy(k):
        part = pl.ds(8 * k if isinstance(k, int) else pl.multiple_of(8 * k, 8), 8)
        return pltpu.make_async_copy(blocks.at[:, part, :], blocks_hbm.at[:, part, :], out_sems.at[k])

    def finish(k):
        highs, lows, members = [], [], []
        for h in range(8):
            b = 8 * k + h
            view = placed[b * 128 : b * 128 + 128, :].T
            x = view[:FIELDS]
            m = view[FIELDS : FIELDS + 1]
            by_row[pl.ds(b, FIELDS, stride=BLK_DEV), :] = x
            block_mass[b : b + 1, :] = m
            forest = view[FIELDS + 2 : FIELDS + 3].astype(jnp.int32)
            members.append((owned == forest).astype(jnp.float32).astype(jnp.bfloat16))
            scaled = m * x
            terms = jnp.concatenate([scaled, scaled * x, jnp.broadcast_to(m, (8, 128))], axis=0)
            high = terms.astype(jnp.bfloat16)
            highs.append(high)
            lows.append((terms - high.astype(jnp.float32)).astype(jnp.bfloat16))
        out_copy(k).start()
        member = jnp.concatenate(members, axis=1)
        for part in (highs, lows):
            acc[...] += lax.dot_general(
                jnp.concatenate(part, axis=1),
                member,
                (((1,), (1,)), ((), ())),
                preferred_element_type=jnp.float32,
            )

    for k in range(BLK_DEV // 8):
        finish(k)
    others = [
        pltpu.make_async_copy(src, dst, out_sems.at[BLK_DEV // 8 + n])
        for n, (src, dst) in enumerate(
            ((block_mass, block_mass_hbm), (fmass, fmass_hbm), (fmean, fmean_hbm), (fsecond, fsecond_hbm))
        )
    ]
    others[0].start()
    weight = acc[2 * FIELDS : 2 * FIELDS + 1]
    mass_total = jnp.broadcast_to(total[0:1, 127:128], (1, FOR_DEV))
    fmass[...] = weight * (FOR_DEV * PEERS / mass_total)
    others[1].start()
    fmean[...] = acc[:FIELDS] / weight
    others[2].start()
    fsecond[...] = acc[FIELDS : 2 * FIELDS] / weight
    others[3].start()
    for copy in [out_copy(k) for k in range(BLK_DEV // 8)] + others:
        copy.wait()


def pack(records, halo_mass, forest_id, dest_block, dest_slot):
    snaps, halos = halo_mass.shape
    groups = snaps * halos // 128

    def by_group(a):
        lead = a.shape[:-2]
        a = a.reshape(lead + (snaps, halos // 128, 128))
        return jnp.swapaxes(a, -3, -2).reshape(-1, 128)

    records, mass, forest, block, slot = map(by_group, (records, halo_mass, forest_id, dest_block, dest_slot))
    row = (groups, 128)
    vmem = pl.BlockSpec(memory_space=pltpu.VMEM)
    params = pltpu.CompilerParams(vmem_limit_bytes=VMEM_LIMIT)
    before, placed, slots = pl.pallas_call(
        init_kernel,
        out_shape=(
            jax.ShapeDtypeStruct((256, 384), jnp.bfloat16),
            jax.ShapeDtypeStruct((PEERS * CAP, 128), jnp.float32),
            jax.ShapeDtypeStruct((SLOTS + 128, 128), jnp.float32),
        ),
        out_specs=(vmem,) * 3,
        cost_estimate=pl.CostEstimate(flops=2**31, bytes_accessed=2**16, transcendentals=0),
        compiler_params=params,
        name="init",
    )()
    target, first_tag = pl.pallas_call(
        rank_kernel,
        out_shape=(jax.ShapeDtypeStruct(row, jnp.int32),) * 2,
        in_specs=[vmem] * 2,
        out_specs=(vmem,) * 2,
        cost_estimate=pl.CostEstimate(flops=2**20, bytes_accessed=2**16, transcendentals=0),
        compiler_params=params,
        name="rank",
    )(block, before)
    outbox, _ = pl.pallas_call(
        pack_kernel,
        out_shape=(
            jax.ShapeDtypeStruct((PEERS, ROWS, 128), jnp.float32),
            jax.ShapeDtypeStruct((PEERS * CAP, 128), jnp.float32),
        ),
        in_specs=[vmem] * 8,
        out_specs=(vmem, pl.BlockSpec(memory_space=pltpu.VMEM)),
        input_output_aliases={7: 1},
        scratch_shapes=[
            pltpu.VMEM(row, jnp.int32),
            pltpu.VMEM((FIELDS * PITCH, 128), jnp.float32),
            [pltpu.VMEM((128, 128), jnp.float32)] * 4,
            [pltpu.SMEM((8, 128), jnp.int32)] * (groups // 8),
            pltpu.SemaphoreType.DMA((groups // 8,)),
        ],
        compiler_params=params,
        name="pack",
    )(target, first_tag, records, mass, forest, block, slot, placed)
    return outbox, slots


def place(msg, slots):
    f32 = jnp.float32
    vmem = pl.BlockSpec(memory_space=pltpu.VMEM)
    shapes = ((FIELDS, BLK_DEV, 128), (BLK_DEV, 128), (1, FOR_DEV), (FIELDS, FOR_DEV), (FIELDS, FOR_DEV))
    return pl.pallas_call(
        place_kernel,
        out_shape=tuple(jax.ShapeDtypeStruct(shape, f32) for shape in shapes + (slots.shape,)),
        in_specs=[vmem] * 2,
        out_specs=(pl.BlockSpec(memory_space=pltpu.HBM),) * 5 + (vmem,),
        input_output_aliases={1: 5},
        scratch_shapes=[pltpu.VMEM(shape, f32) for shape in shapes]
        + [
            pltpu.VMEM((2 * FIELDS + 8, FOR_DEV), f32),
            [pltpu.VMEM((CAP, 128), f32)] * 4,
            pltpu.VMEM((PEERS, 128), jnp.int32),
            [pltpu.SMEM((8, 128), jnp.int32)] * (PEERS // 8),
            pltpu.SemaphoreType.DMA((PEERS // 8,)),
            pltpu.SemaphoreType.DMA((BLK_DEV // 8 + 4,)),
        ],
        compiler_params=pltpu.CompilerParams(vmem_limit_bytes=VMEM_LIMIT),
        name="place",
    )(msg, slots)[:5]


def on_device(records, halo_mass, forest_id, dest_block, dest_slot):
    outbox, slots = pack(records, halo_mass, forest_id, dest_block, dest_slot)
    inbox = lax.all_to_all(outbox, EXCHANGE, split_axis=0, concat_axis=0, tiled=True)
    blocks, block_mass, fmass, fmean, fsecond = place(inbox, slots)
    return blocks, block_mass, fmass.reshape(FOR_DEV), fmean, fsecond


def solution(mesh):
    split = Mesh(
        mesh.devices.reshape(mesh.shape["row"], mesh.shape["sa"], 2, 2, 2, 2),
        ROW_SA_HA,
    )
    in_specs = (
        P(None, "sa", ROW_HA),
        P("sa", ROW_HA),
        P("sa", ROW_HA),
        P("sa", ROW_HA),
        P("sa", ROW_HA),
    )
    out_specs = (
        P(None, ROW_SA_HA, None),
        P(ROW_SA_HA, None),
        P(ROW_SA_HA),
        P(None, ROW_SA_HA),
        P(None, ROW_SA_HA),
    )
    return jax.shard_map(
        on_device, mesh=split, in_specs=in_specs, out_specs=out_specs, check_vma=False
    )
```

```python
import jax
import jax.numpy as jnp
from jax import lax
from jax.experimental import pallas as pl
from jax.experimental.pallas import tpu as pltpu
from jax.sharding import Mesh
from jax.sharding import PartitionSpec as P

FIELDS = 64
FOR_DEV = 128
BLK_DEV = 40
SLOTS = BLK_DEV * 128
PEERS = 64
CAP = 88
ROWS = 48
TAGS = 48
PITCH = 40
VMEM_LIMIT = 24 * 1024 * 1024
EXCHANGE = ("core", "sa", "z0", "z1", "z2")
ROW_HA = ("row", "z2", "z1", "z0", "core")
ROW_SA_HA = ("row", "sa", "z2", "z1", "z0", "core")


def iota(shape, dim):
    return lax.broadcasted_iota(jnp.int32, shape, dim)


def owner_of(block):
    return lax.shift_right_logical(block * 1639, 16)


def position_of(owner):
    core = (owner & 1) << 5
    plane = lax.shift_right_logical(owner, 4) << 3
    turned = ((owner & 2) << 1) | lax.shift_right_logical(owner & 4, 1) | lax.shift_right_logical(owner & 8, 3)
    return core | plane | turned


def init_kernel(before, outbox, slots):
    ordered = (iota((256, 384), 0) < iota((256, 384), 1)) | (iota((256, 384), 1) >= 256)
    before[...] = ordered.astype(jnp.float32).astype(jnp.bfloat16)

    for array in (outbox, slots):

        def clear(k, carry):
            array[pl.ds(pl.multiple_of(k * 128, 128), 128), :] = jnp.zeros((128, 128), jnp.float32)
            return carry

        lax.fori_loop(0, array.shape[0] // 128, clear, 0)


def rank_kernel(block, before, target, first_tag):
    groups = block.shape[0]
    peer = iota((PEERS, 128), 0)
    base = jnp.zeros((PEERS, 128), jnp.float32)
    goal = position_of(owner_of(block[...]))
    for g in range(0, groups, 2):
        member = jnp.concatenate([peer == goal[g : g + 1], peer == goal[g + 1 : g + 2]], axis=1)
        counts = jnp.dot(
            member.astype(jnp.float32).astype(jnp.bfloat16), before[...], preferred_element_type=jnp.float32
        )
        rank = counts[:, :256] + jnp.concatenate([base, base], axis=1)
        rank = jnp.sum(jnp.where(member, rank, 0.0), axis=0, keepdims=True).astype(jnp.int32)
        base = base + counts[:, 256:]
        first_tag[g : g + 1, :] = rank[:, :128]
        first_tag[g + 1 : g + 2, :] = rank[:, 128:]
    rank = first_tag[...]
    target[...] = goal * CAP + rank
    first_tag[...] = lax.shift_right_logical(rank, 3) << 2


def pack_kernel(
    target_v, first_tag, rec, mass, forest, block, slot_in, start, out, placed, slot, spaced, tiles, target_s, sems
):
    del start
    groups = mass.shape[0]

    def index_copy(k):
        return pltpu.make_async_copy(target_v.at[8 * k : 8 * k + 8, :], target_s[k], sems.at[k])

    for k in range(groups // 8):
        index_copy(k).start()
    for tile in tiles:
        tile[...] = jnp.zeros_like(tile)
    slot[...] = (block[...] - owner_of(block[...]) * BLK_DEV) * 128 + slot_in[...] + 1

    for f in range(FIELDS):
        spaced[PITCH * f : PITCH * f + groups, :] = rec[groups * f : groups * f + groups, :]
    line = iota((TAGS, 128), 0)

    def turn(group, tile):
        def row(ref):
            return jnp.broadcast_to(ref[pl.ds(group, 1), :], (TAGS, 128))

        own_line = line - row(first_tag)
        tags = jnp.where(own_line == 0, row(mass), 0.0)
        tags = jnp.where(own_line == 1, row(slot).astype(jnp.float32), tags)
        tags = jnp.where(own_line == 2, (row(forest) & (FOR_DEV - 1)).astype(jnp.float32), tags)
        stack = jnp.concatenate([spaced[pl.ds(group, FIELDS, stride=PITCH), :], tags], axis=0)
        tile[:, : FIELDS + TAGS] = stack.T

    turn(0, tiles[0])

    for i in range(groups):
        if i % 8 == 0:
            index_copy(i // 8).wait()
        if i + 1 < groups:
            turn(i + 1, tiles[(i + 1) % 4])
        tile = tiles[i % 4]
        for r in range(128):
            placed[pl.ds(target_s[i // 8][i % 8, r], 1), :] = tile[r : r + 1, :]

    lane = iota((8, 128), 1)
    low = lane < FIELDS
    total = jnp.sum(jnp.sum(mass[...], axis=0, keepdims=True), axis=1, keepdims=True)
    corner = jnp.where(lane == 127, jnp.broadcast_to(total, (8, 128)), 0.0)

    for p in range(PEERS):
        rows = [placed[CAP * p + 8 * v : CAP * p + 8 * v + 8, :] for v in range(CAP // 8)]
        for v in range(5):
            out[p, 8 * v : 8 * v + 8, :] = jnp.where(low, rows[v], pltpu.roll(rows[v + 6], 64, 1))
        tags = corner
        for row in rows:
            tags = tags + row
        out[p, 40:48, :] = jnp.where(low, rows[5], tags)


def place_kernel(
    msg, start, blocks_hbm, block_mass_hbm, fmass_hbm, fmean_hbm, fsecond_hbm, placed,
    blocks, block_mass, fmass, fmean, fsecond, acc, tiles, slot_v, slot_s, sems, out_sems,
):
    del start
    by_row = blocks.reshape(FIELDS * BLK_DEV, 128)

    def index_copy(g):
        return pltpu.make_async_copy(slot_v.at[8 * g : 8 * g + 8, :], slot_s[g], sems.at[g])

    lane = iota((8, 128), 1)
    low = lane < FIELDS
    slot_lane = (lane >= FIELDS) & (lane < FIELDS + 4 * (CAP // 8)) & (lane % 4 == 1)
    total = jnp.zeros((8, 128), jnp.float32)
    for g in range(PEERS // 8):
        index = jnp.zeros((8, 128), jnp.float32)
        for k in range(8):
            tags = msg[8 * g + k, 40:48, :]
            total = total + tags
            index = index + pltpu.roll(
                jnp.where(slot_lane, tags, 0.0), (64 * (k // 4) + k % 4 - 65) % 128, 1
            )
        index = index.astype(jnp.int32)
        slot_v[8 * g : 8 * g + 8, :] = jnp.where(index == 0, SLOTS, index - 1)
        index_copy(g).start()
    acc[...] = jnp.zeros_like(acc)

    def turn(p, tile):
        tags = msg[p, 40:48, :]
        for v in range(CAP // 8):
            if v < 6:
                own = msg[p, 8 * v : 8 * v + 8, :]
            else:
                own = pltpu.roll(msg[p, 8 * v - 48 : 8 * v - 40, :], 64, 1)
            side = pltpu.roll(tags, 128 - 4 * v, 1) if v else tags
            tile[8 * v : 8 * v + 8, :] = jnp.where(low, own, side)

    turn(0, tiles[0])
    turn(1, tiles[1])

    for i in range(PEERS):
        if i == 0:
            index_copy(0).wait()
        if i == 8:
            for g in range(1, PEERS // 8):
                index_copy(g).wait()
        if i + 2 < PEERS:
            turn(i + 2, tiles[(i + 2) % 4])
        tile = tiles[i % 4]
        for r in range(CAP):
            col = r // 8 * 4 + i % 8 % 4 + i % 8 // 4 * 64
            placed[pl.ds(slot_s[i // 8][r % 8, col], 1), :] = tile[r : r + 1, :]

    owned = iota((FOR_DEV, 128), 0)

    def out_copy(k):
        part = pl.ds(8 * k if isinstance(k, int) else pl.multiple_of(8 * k, 8), 8)
        return pltpu.make_async_copy(blocks.at[:, part, :], blocks_hbm.at[:, part, :], out_sems.at[k])

    def finish(k):
        highs, lows, members = [], [], []
        for h in range(8):
            b = 8 * k + h
            view = placed[b * 128 : b * 128 + 128, :].T
            x = view[:FIELDS]
            m = view[FIELDS : FIELDS + 1]
            by_row[pl.ds(b, FIELDS, stride=BLK_DEV), :] = x
            block_mass[b : b + 1, :] = m
            forest = view[FIELDS + 2 : FIELDS + 3].astype(jnp.int32)
            members.append((owned == forest).astype(jnp.float32).astype(jnp.bfloat16))
            scaled = m * x
            terms = jnp.concatenate([scaled, scaled * x, jnp.broadcast_to(m, (8, 128))], axis=0)
            high = terms.astype(jnp.bfloat16)
            highs.append(high)
            lows.append((terms - high.astype(jnp.float32)).astype(jnp.bfloat16))
        out_copy(k).start()
        member = jnp.concatenate(members, axis=1)
        for part in (highs, lows):
            acc[...] += lax.dot_general(
                jnp.concatenate(part, axis=1),
                member,
                (((1,), (1,)), ((), ())),
                preferred_element_type=jnp.float32,
            )

    for k in range(BLK_DEV // 8):
        finish(k)
    others = [
        pltpu.make_async_copy(src, dst, out_sems.at[BLK_DEV // 8 + n])
        for n, (src, dst) in enumerate(
            ((block_mass, block_mass_hbm), (fmass, fmass_hbm), (fmean, fmean_hbm), (fsecond, fsecond_hbm))
        )
    ]
    others[0].start()
    weight = acc[2 * FIELDS : 2 * FIELDS + 1]
    mass_total = jnp.broadcast_to(total[0:1, 127:128], (1, FOR_DEV))
    fmass[...] = weight * (FOR_DEV * PEERS / mass_total)
    others[1].start()
    fmean[...] = acc[:FIELDS] / weight
    others[2].start()
    fsecond[...] = acc[FIELDS : 2 * FIELDS] / weight
    others[3].start()
    for copy in [out_copy(k) for k in range(BLK_DEV // 8)] + others:
        copy.wait()


def pack(records, halo_mass, forest_id, dest_block, dest_slot):
    snaps, halos = halo_mass.shape
    groups = snaps * halos // 128

    def by_group(a):
        lead = a.shape[:-2]
        a = a.reshape(lead + (snaps, halos // 128, 128))
        return jnp.swapaxes(a, -3, -2).reshape(-1, 128)

    records, mass, forest, block, slot = map(by_group, (records, halo_mass, forest_id, dest_block, dest_slot))
    row = (groups, 128)
    vmem = pl.BlockSpec(memory_space=pltpu.VMEM)
    params = pltpu.CompilerParams(vmem_limit_bytes=VMEM_LIMIT)
    before, placed, slots = pl.pallas_call(
        init_kernel,
        out_shape=(
            jax.ShapeDtypeStruct((256, 384), jnp.bfloat16),
            jax.ShapeDtypeStruct((PEERS * CAP, 128), jnp.float32),
            jax.ShapeDtypeStruct((SLOTS + 128, 128), jnp.float32),
        ),
        out_specs=(vmem,) * 3,
        cost_estimate=pl.CostEstimate(flops=2**31, bytes_accessed=2**16, transcendentals=0),
        compiler_params=params,
        name="init",
    )()
    target, first_tag = pl.pallas_call(
        rank_kernel,
        out_shape=(jax.ShapeDtypeStruct(row, jnp.int32),) * 2,
        in_specs=[vmem] * 2,
        out_specs=(vmem,) * 2,
        cost_estimate=pl.CostEstimate(flops=2**20, bytes_accessed=2**16, transcendentals=0),
        compiler_params=params,
        name="rank",
    )(block, before)
    outbox, _ = pl.pallas_call(
        pack_kernel,
        out_shape=(
            jax.ShapeDtypeStruct((PEERS, ROWS, 128), jnp.float32),
            jax.ShapeDtypeStruct((PEERS * CAP, 128), jnp.float32),
        ),
        in_specs=[vmem] * 8,
        out_specs=(vmem, pl.BlockSpec(memory_space=pltpu.VMEM)),
        input_output_aliases={7: 1},
        scratch_shapes=[
            pltpu.VMEM(row, jnp.int32),
            pltpu.VMEM((FIELDS * PITCH, 128), jnp.float32),
            [pltpu.VMEM((128, 128), jnp.float32)] * 4,
            [pltpu.SMEM((8, 128), jnp.int32)] * (groups // 8),
            pltpu.SemaphoreType.DMA((groups // 8,)),
        ],
        compiler_params=params,
        name="pack",
    )(target, first_tag, records, mass, forest, block, slot, placed)
    return outbox, slots


def place(msg, slots):
    f32 = jnp.float32
    vmem = pl.BlockSpec(memory_space=pltpu.VMEM)
    shapes = ((FIELDS, BLK_DEV, 128), (BLK_DEV, 128), (1, FOR_DEV), (FIELDS, FOR_DEV), (FIELDS, FOR_DEV))
    return pl.pallas_call(
        place_kernel,
        out_shape=tuple(jax.ShapeDtypeStruct(shape, f32) for shape in shapes + (slots.shape,)),
        in_specs=[vmem] * 2,
        out_specs=(pl.BlockSpec(memory_space=pltpu.HBM),) * 5 + (vmem,),
        input_output_aliases={1: 5},
        scratch_shapes=[pltpu.VMEM(shape, f32) for shape in shapes]
        + [
            pltpu.VMEM((2 * FIELDS + 8, FOR_DEV), f32),
            [pltpu.VMEM((CAP, 128), f32)] * 4,
            pltpu.VMEM((PEERS, 128), jnp.int32),
            [pltpu.SMEM((8, 128), jnp.int32)] * (PEERS // 8),
            pltpu.SemaphoreType.DMA((PEERS // 8,)),
            pltpu.SemaphoreType.DMA((BLK_DEV // 8 + 4,)),
        ],
        compiler_params=pltpu.CompilerParams(vmem_limit_bytes=VMEM_LIMIT),
        name="place",
    )(msg, slots)[:5]


def on_device(records, halo_mass, forest_id, dest_block, dest_slot):
    outbox, slots = pack(records, halo_mass, forest_id, dest_block, dest_slot)
    inbox = lax.all_to_all(outbox, EXCHANGE, split_axis=0, concat_axis=0, tiled=True)
    blocks, block_mass, fmass, fmean, fsecond = place(inbox, slots)
    return blocks, block_mass, fmass.reshape(FOR_DEV), fmean, fsecond


def solution(mesh):
    split = Mesh(
        mesh.devices.reshape(mesh.shape["row"], mesh.shape["sa"], 2, 2, 2, 2),
        ROW_SA_HA,
    )
    in_specs = (
        P(None, "sa", ROW_HA),
        P("sa", ROW_HA),
        P("sa", ROW_HA),
        P("sa", ROW_HA),
        P("sa", ROW_HA),
    )
    out_specs = (
        P(None, ROW_SA_HA, None),
        P(ROW_SA_HA, None),
        P(ROW_SA_HA),
        P(None, ROW_SA_HA),
        P(None, ROW_SA_HA),
    )
    return jax.shard_map(
        on_device, mesh=split, in_specs=in_specs, out_specs=out_specs, check_vma=False
    )
```

```python
import jax
import jax.numpy as jnp
from jax import lax
from jax.experimental import pallas as pl
from jax.experimental.pallas import tpu as pltpu
from jax.sharding import Mesh
from jax.sharding import PartitionSpec as P

FIELDS = 64
FOR_DEV = 128
BLK_DEV = 40
SLOTS = BLK_DEV * 128
PEERS = 64
CAP = 88
ROWS = 48
TAGS = 48
PITCH = 40
VMEM_LIMIT = 24 * 1024 * 1024
EXCHANGE = ("core", "sa", "z0", "z1", "z2")
ROW_HA = ("row", "z2", "z1", "z0", "core")
ROW_SA_HA = ("row", "sa", "z2", "z1", "z0", "core")


def iota(shape, dim):
    return lax.broadcasted_iota(jnp.int32, shape, dim)


def owner_of(block):
    return lax.shift_right_logical(block * 1639, 16)


def position_of(owner):
    core = (owner & 1) << 5
    plane = lax.shift_right_logical(owner, 4) << 3
    turned = ((owner & 2) << 1) | lax.shift_right_logical(owner & 4, 1) | lax.shift_right_logical(owner & 8, 3)
    return core | plane | turned


def init_kernel(before, outbox, slots):
    ordered = (iota((256, 384), 0) < iota((256, 384), 1)) | (iota((256, 384), 1) >= 256)
    before[...] = ordered.astype(jnp.float32).astype(jnp.bfloat16)

    for array in (outbox, slots):

        def clear(k, carry):
            array[pl.ds(pl.multiple_of(k * 128, 128), 128), :] = jnp.zeros((128, 128), jnp.float32)
            return carry

        lax.fori_loop(0, array.shape[0] // 128, clear, 0)


def rank_kernel(block, before, target, first_tag):
    groups = block.shape[0]
    peer = iota((PEERS, 128), 0)
    base = jnp.zeros((PEERS, 128), jnp.float32)
    goal = position_of(owner_of(block[...]))
    for g in range(0, groups, 2):
        member = jnp.concatenate([peer == goal[g : g + 1], peer == goal[g + 1 : g + 2]], axis=1)
        counts = jnp.dot(
            member.astype(jnp.float32).astype(jnp.bfloat16), before[...], preferred_element_type=jnp.float32
        )
        rank = counts[:, :256] + jnp.concatenate([base, base], axis=1)
        rank = jnp.sum(jnp.where(member, rank, 0.0), axis=0, keepdims=True).astype(jnp.int32)
        base = base + counts[:, 256:]
        first_tag[g : g + 1, :] = rank[:, :128]
        first_tag[g + 1 : g + 2, :] = rank[:, 128:]
    rank = first_tag[...]
    target[...] = goal * CAP + rank
    first_tag[...] = lax.shift_right_logical(rank, 3) << 2


def pack_kernel(
    target_v, first_tag, rec, mass, forest, block, slot_in, start, out, placed, slot, spaced, tiles, target_s, sems
):
    del start
    groups = mass.shape[0]

    def index_copy(k):
        return pltpu.make_async_copy(target_v.at[8 * k : 8 * k + 8, :], target_s[k], sems.at[k])

    for k in range(groups // 8):
        index_copy(k).start()
    for tile in tiles:
        tile[...] = jnp.zeros_like(tile)
    slot[...] = (block[...] - owner_of(block[...]) * BLK_DEV) * 128 + slot_in[...] + 1

    for f in range(FIELDS):
        spaced[PITCH * f : PITCH * f + groups, :] = rec[groups * f : groups * f + groups, :]
    line = iota((TAGS, 128), 0)

    def turn(group, tile):
        def row(ref):
            return jnp.broadcast_to(ref[pl.ds(group, 1), :], (TAGS, 128))

        own_line = line - row(first_tag)
        tags = jnp.where(own_line == 0, row(mass), 0.0)
        tags = jnp.where(own_line == 1, row(slot).astype(jnp.float32), tags)
        tags = jnp.where(own_line == 2, (row(forest) & (FOR_DEV - 1)).astype(jnp.float32), tags)
        stack = jnp.concatenate([spaced[pl.ds(group, FIELDS, stride=PITCH), :], tags], axis=0)
        tile[:, : FIELDS + TAGS] = stack.T

    turn(0, tiles[0])

    for i in range(groups):
        if i % 8 == 0:
            index_copy(i // 8).wait()
        if i + 1 < groups:
            turn(i + 1, tiles[(i + 1) % 4])
        tile = tiles[i % 4]
        for r in range(128):
            placed[pl.ds(target_s[i // 8][i % 8, r], 1), :] = tile[r : r + 1, :]

    lane = iota((8, 128), 1)
    low = lane < FIELDS
    total = jnp.sum(jnp.sum(mass[...], axis=0, keepdims=True), axis=1, keepdims=True)
    corner = jnp.where(lane == 127, jnp.broadcast_to(total, (8, 128)), 0.0)

    for p in range(PEERS):
        rows = [placed[CAP * p + 8 * v : CAP * p + 8 * v + 8, :] for v in range(CAP // 8)]
        for v in range(5):
            out[p, 8 * v : 8 * v + 8, :] = jnp.where(low, rows[v], pltpu.roll(rows[v + 6], 64, 1))
        tags = corner
        for row in rows:
            tags = tags + row
        out[p, 40:48, :] = jnp.where(low, rows[5], tags)


def place_kernel(
    msg, start, blocks_hbm, block_mass_hbm, fmass_hbm, fmean_hbm, fsecond_hbm, placed,
    blocks, block_mass, fmass, fmean, fsecond, acc, tiles, slot_v, slot_s, sems, out_sems,
):
    del start
    by_row = blocks.reshape(FIELDS * BLK_DEV, 128)

    def index_copy(g):
        return pltpu.make_async_copy(slot_v.at[8 * g : 8 * g + 8, :], slot_s[g], sems.at[g])

    lane = iota((8, 128), 1)
    low = lane < FIELDS
    slot_lane = (lane >= FIELDS) & (lane < FIELDS + 4 * (CAP // 8)) & (lane % 4 == 1)
    total = jnp.zeros((8, 128), jnp.float32)
    for g in range(PEERS // 8):
        index = jnp.zeros((8, 128), jnp.float32)
        for k in range(8):
            tags = msg[8 * g + k, 40:48, :]
            total = total + tags
            index = index + pltpu.roll(
                jnp.where(slot_lane, tags, 0.0), (64 * (k // 4) + k % 4 - 65) % 128, 1
            )
        index = index.astype(jnp.int32)
        slot_v[8 * g : 8 * g + 8, :] = jnp.where(index == 0, SLOTS, index - 1)
        index_copy(g).start()
    acc[...] = jnp.zeros_like(acc)

    def turn(p, tile):
        tags = msg[p, 40:48, :]
        for v in range(CAP // 8):
            if v < 6:
                own = msg[p, 8 * v : 8 * v + 8, :]
            else:
                own = pltpu.roll(msg[p, 8 * v - 48 : 8 * v - 40, :], 64, 1)
            side = pltpu.roll(tags, 128 - 4 * v, 1) if v else tags
            tile[8 * v : 8 * v + 8, :] = jnp.where(low, own, side)

    for i in range(6):
        turn(i, tiles[i])

    for i in range(PEERS):
        if i == 0:
            index_copy(0).wait()
        if i == 8:
            for g in range(1, PEERS // 8):
                index_copy(g).wait()
        if i + 6 < PEERS:
            turn(i + 6, tiles[(i + 6) % 8])
        tile = tiles[i % 8]
        for r in range(CAP):
            col = r // 8 * 4 + i % 8 % 4 + i % 8 // 4 * 64
            placed[pl.ds(slot_s[i // 8][r % 8, col], 1), :] = tile[r : r + 1, :]

    owned = iota((FOR_DEV, 128), 0)

    def out_copy(k):
        part = pl.ds(8 * k if isinstance(k, int) else pl.multiple_of(8 * k, 8), 8)
        return pltpu.make_async_copy(blocks.at[:, part, :], blocks_hbm.at[:, part, :], out_sems.at[k])

    def finish(k):
        highs, lows, members = [], [], []
        for h in range(8):
            b = 8 * k + h
            view = placed[b * 128 : b * 128 + 128, :].T
            x = view[:FIELDS]
            m = view[FIELDS : FIELDS + 1]
            by_row[pl.ds(b, FIELDS, stride=BLK_DEV), :] = x
            block_mass[b : b + 1, :] = m
            forest = view[FIELDS + 2 : FIELDS + 3].astype(jnp.int32)
            members.append((owned == forest).astype(jnp.float32).astype(jnp.bfloat16))
            scaled = m * x
            terms = jnp.concatenate([scaled, scaled * x, jnp.broadcast_to(m, (8, 128))], axis=0)
            high = terms.astype(jnp.bfloat16)
            highs.append(high)
            lows.append((terms - high.astype(jnp.float32)).astype(jnp.bfloat16))
        out_copy(k).start()
        member = jnp.concatenate(members, axis=1)
        for part in (highs, lows):
            acc[...] += lax.dot_general(
                jnp.concatenate(part, axis=1),
                member,
                (((1,), (1,)), ((), ())),
                preferred_element_type=jnp.float32,
            )

    for k in range(BLK_DEV // 8):
        finish(k)
    others = [
        pltpu.make_async_copy(src, dst, out_sems.at[BLK_DEV // 8 + n])
        for n, (src, dst) in enumerate(
            ((block_mass, block_mass_hbm), (fmass, fmass_hbm), (fmean, fmean_hbm), (fsecond, fsecond_hbm))
        )
    ]
    others[0].start()
    weight = acc[2 * FIELDS : 2 * FIELDS + 1]
    mass_total = jnp.broadcast_to(total[0:1, 127:128], (1, FOR_DEV))
    fmass[...] = weight * (FOR_DEV * PEERS / mass_total)
    others[1].start()
    fmean[...] = acc[:FIELDS] / weight
    others[2].start()
    fsecond[...] = acc[FIELDS : 2 * FIELDS] / weight
    others[3].start()
    for copy in [out_copy(k) for k in range(BLK_DEV // 8)] + others:
        copy.wait()


def pack(records, halo_mass, forest_id, dest_block, dest_slot):
    snaps, halos = halo_mass.shape
    groups = snaps * halos // 128

    def by_group(a):
        lead = a.shape[:-2]
        a = a.reshape(lead + (snaps, halos // 128, 128))
        return jnp.swapaxes(a, -3, -2).reshape(-1, 128)

    records, mass, forest, block, slot = map(by_group, (records, halo_mass, forest_id, dest_block, dest_slot))
    row = (groups, 128)
    vmem = pl.BlockSpec(memory_space=pltpu.VMEM)
    params = pltpu.CompilerParams(vmem_limit_bytes=VMEM_LIMIT)
    before, placed, slots = pl.pallas_call(
        init_kernel,
        out_shape=(
            jax.ShapeDtypeStruct((256, 384), jnp.bfloat16),
            jax.ShapeDtypeStruct((PEERS * CAP, 128), jnp.float32),
            jax.ShapeDtypeStruct((SLOTS + 128, 128), jnp.float32),
        ),
        out_specs=(vmem,) * 3,
        cost_estimate=pl.CostEstimate(flops=2**31, bytes_accessed=2**16, transcendentals=0),
        compiler_params=params,
        name="init",
    )()
    target, first_tag = pl.pallas_call(
        rank_kernel,
        out_shape=(jax.ShapeDtypeStruct(row, jnp.int32),) * 2,
        in_specs=[vmem] * 2,
        out_specs=(vmem,) * 2,
        cost_estimate=pl.CostEstimate(flops=2**20, bytes_accessed=2**16, transcendentals=0),
        compiler_params=params,
        name="rank",
    )(block, before)
    outbox, _ = pl.pallas_call(
        pack_kernel,
        out_shape=(
            jax.ShapeDtypeStruct((PEERS, ROWS, 128), jnp.float32),
            jax.ShapeDtypeStruct((PEERS * CAP, 128), jnp.float32),
        ),
        in_specs=[vmem] * 8,
        out_specs=(vmem, pl.BlockSpec(memory_space=pltpu.VMEM)),
        input_output_aliases={7: 1},
        scratch_shapes=[
            pltpu.VMEM(row, jnp.int32),
            pltpu.VMEM((FIELDS * PITCH, 128), jnp.float32),
            [pltpu.VMEM((128, 128), jnp.float32)] * 4,
            [pltpu.SMEM((8, 128), jnp.int32)] * (groups // 8),
            pltpu.SemaphoreType.DMA((groups // 8,)),
        ],
        compiler_params=params,
        name="pack",
    )(target, first_tag, records, mass, forest, block, slot, placed)
    return outbox, slots


def place(msg, slots):
    f32 = jnp.float32
    vmem = pl.BlockSpec(memory_space=pltpu.VMEM)
    shapes = ((FIELDS, BLK_DEV, 128), (BLK_DEV, 128), (1, FOR_DEV), (FIELDS, FOR_DEV), (FIELDS, FOR_DEV))
    return pl.pallas_call(
        place_kernel,
        out_shape=tuple(jax.ShapeDtypeStruct(shape, f32) for shape in shapes + (slots.shape,)),
        in_specs=[vmem] * 2,
        out_specs=(pl.BlockSpec(memory_space=pltpu.HBM),) * 5 + (vmem,),
        input_output_aliases={1: 5},
        scratch_shapes=[pltpu.VMEM(shape, f32) for shape in shapes]
        + [
            pltpu.VMEM((2 * FIELDS + 8, FOR_DEV), f32),
            [pltpu.VMEM((CAP, 128), f32)] * 8,
            pltpu.VMEM((PEERS, 128), jnp.int32),
            [pltpu.SMEM((8, 128), jnp.int32)] * (PEERS // 8),
            pltpu.SemaphoreType.DMA((PEERS // 8,)),
            pltpu.SemaphoreType.DMA((BLK_DEV // 8 + 4,)),
        ],
        compiler_params=pltpu.CompilerParams(vmem_limit_bytes=VMEM_LIMIT),
        name="place",
    )(msg, slots)[:5]


def on_device(records, halo_mass, forest_id, dest_block, dest_slot):
    outbox, slots = pack(records, halo_mass, forest_id, dest_block, dest_slot)
    inbox = lax.all_to_all(outbox, EXCHANGE, split_axis=0, concat_axis=0, tiled=True)
    blocks, block_mass, fmass, fmean, fsecond = place(inbox, slots)
    return blocks, block_mass, fmass.reshape(FOR_DEV), fmean, fsecond


def solution(mesh):
    split = Mesh(
        mesh.devices.reshape(mesh.shape["row"], mesh.shape["sa"], 2, 2, 2, 2),
        ROW_SA_HA,
    )
    in_specs = (
        P(None, "sa", ROW_HA),
        P("sa", ROW_HA),
        P("sa", ROW_HA),
        P("sa", ROW_HA),
        P("sa", ROW_HA),
    )
    out_specs = (
        P(None, ROW_SA_HA, None),
        P(ROW_SA_HA, None),
        P(ROW_SA_HA),
        P(None, ROW_SA_HA),
        P(None, ROW_SA_HA),
    )
    return jax.shard_map(
        on_device, mesh=split, in_specs=in_specs, out_specs=out_specs, check_vma=False
    )
```
